32 devices in a mesh: section: 2 (over core), dp: 4 (over y, x), seq: 4 (over z).
Axes of the slice: x: 2, y: 2, z: 4, core: 2. Of those that a mesh axis runs over, the one named last changes fastest.
Arguments:
- inputs: bfloat16 [8, 1024, 768], P('dp', 'seq'), may hold values from -8 to 8
- cotangent: bfloat16 [8, 1024, 768], P('dp', 'seq'), may hold values from -6 to 6
- question_positions: int32 [8, 64], P('dp'), may hold values from 0 to 1023, as said below
- question_counts: int32 [8], P('dp'), may hold values from 32 to 64
- query_weight: bfloat16 [2, 768, 768], P('section'), may hold values from -0.21875 to 0.21875
- key_weight: bfloat16 [2, 768, 768], P('section'), may hold values from -0.21875 to 0.21875
- value_weight: bfloat16 [2, 768, 768], P('section'), may hold values from -0.21875 to 0.21875
- output_weight: bfloat16 [2, 768, 768], P('section'), may hold values from -0.875 to 0.875
- up_weight: bfloat16 [2, 768, 3072], P('section'), may hold values from -0.21875 to 0.21875
- down_weight: bfloat16 [2, 3072, 768], P('section'), may hold values from -0.109375 to 0.109375
- key_pool: float32 [2, 5, 768], P('section'), may hold values from -2.5 to 2.5
- value_pool: float32 [2, 5, 768], P('section'), may hold values from -2.5 to 2.5
- attn_norm_gain: float32 [2, 768], P('section'), may hold values from 0.5 to 1.5
- attn_norm_bias: float32 [2, 768], P('section'), may hold values from -3 to 3
- ffn_norm_gain: float32 [2, 768], P('section'), may hold values from 0.5 to 1.5
- ffn_norm_bias: float32 [2, 768], P('section'), may hold values from -3 to 3
Outputs:
- section_outputs: bfloat16 [2, 8, 1024, 768], P('section', 'dp', 'seq')
- input_grads: bfloat16 [2, 8, 1024, 768], P('section', 'dp', 'seq')
- query_weight_grad: float32 [2, 768, 768], P('section')
- key_weight_grad: float32 [2, 768, 768], P('section')
- value_weight_grad: float32 [2, 768, 768], P('section')
- output_weight_grad: float32 [2, 768, 768], P('section')
- up_weight_grad: float32 [2, 768, 3072], P('section')
- down_weight_grad: float32 [2, 3072, 768], P('section')
- key_pool_grad: float32 [2, 5, 768], P('section')
- value_pool_grad: float32 [2, 5, 768], P('section')
- attn_norm_gain_grad: float32 [2, 768], P('section')
- attn_norm_bias_grad: float32 [2, 768], P('section')
- ffn_norm_gain_grad: float32 [2, 768], P('section')
- ffn_norm_bias_grad: float32 [2, 768], P('section')
The draws below stay inside these ranges and needn't reach their ends.
Inputs may be any that keep to these rules, and one draw needn't show every extreme that they name: `question_positions`: each item's slots hold consecutive positions, slot c at a per-item start plus c.
All inputs are finite; a program needn't handle non-finite values.
Results may differ from the reference program's by a relative error of at most 0.014.
Values may be sent and summed in bfloat16 or wider, within the bound.
A program may use at most 320 MiB of HBM per device.

```python
import math
import jax
import jax.numpy as jnp
from jax import lax

D = 768
DH = 64
FF = 3072
WIN = 128
PWIN = 512
KERNEL = 5
STRIDE = 4
QMAX = 64
LAYERS = 2
ITEMS = 8
LENGTH = 1024


def draw_question_counts(key, part):
    counts = jax.random.randint(key, (ITEMS,), QMAX // 2, QMAX + 1)
    counts = counts.at[0].set(QMAX).at[1].set(QMAX // 2)
    return counts.astype(jnp.int32)


def draw_question_positions(key, part):
    starts = jax.random.randint(key, (ITEMS,), 0, LENGTH - QMAX + 1)
    starts = starts.at[0].set(LENGTH - QMAX).at[1].set(0)
    return (starts[:, None] + jnp.arange(QMAX, dtype=jnp.int32)[None, :]).astype(jnp.int32)


def draw_inputs(key, part):
    noise_key, direction_key = jax.random.split(jax.random.fold_in(key, 11))
    direction = jax.random.normal(direction_key, (ITEMS, 1, D), jnp.float32)
    ramp = (jnp.arange(LENGTH, dtype=jnp.float32) / LENGTH)[None, :, None]
    noise = jax.random.normal(noise_key, (ITEMS, LENGTH, D), jnp.float32)
    amplitude = 1.2
    return jnp.clip(noise + amplitude * ramp * direction, -8.0, 8.0).astype(jnp.bfloat16)


def levels(own_key, extent, cuts, least, high):
    def one(axis_at, shards_of):
        draws = jax.random.uniform(jax.random.fold_in(jax.random.fold_in(own_key, 6), axis_at), (shards_of,), jnp.float32, least / len(cuts), high / len(cuts))
        return jnp.repeat(jnp.exp(draws), extent[axis_at] // shards_of).reshape((-1,) + (1,) * (len(extent) - axis_at - 1))

    factor_of = one(*cuts[0])
    for cut in cuts[1:]:
        factor_of = factor_of * one(*cut)
    return factor_of


def scatter_about(rng, extent, scale, limit, pieces=(), kind=jnp.bfloat16):
    values = jax.random.normal(rng, extent, jnp.float32) * scale
    if len(pieces) > 0:
        values = levels(rng, extent, pieces, -0.22, 0.18) * values
    return jnp.clip(values, min=-limit, max=limit).astype(kind)


def setup_inputs(seed: int = 0) -> dict:
    streams_of = jax.random.split(jax.random.key(seed), 17)
    return {
        "inputs": draw_inputs(jax.random.fold_in(streams_of[16], 71), 0),
        "cotangent": scatter_about(streams_of[1], (ITEMS, LENGTH, D), 1.0, 6.0, ((0, 4), (1, 4))),
        "question_positions": draw_question_positions(jax.random.fold_in(streams_of[16], 71), 0),
        "question_counts": draw_question_counts(jax.random.fold_in(streams_of[16], 71), 0),
        "query_weight": scatter_about(streams_of[4], (LAYERS, D, D), D ** -0.5, 0.21875, ((0, 2),)),
        "key_weight": scatter_about(streams_of[5], (LAYERS, D, D), D ** -0.5, 0.21875, ((0, 2),)),
        "value_weight": scatter_about(streams_of[6], (LAYERS, D, D), D ** -0.5, 0.21875, ((0, 2),)),
        "output_weight": scatter_about(streams_of[7], (LAYERS, D, D), (D // 16) ** -0.5, 0.875, ((0, 2),)),
        "up_weight": scatter_about(streams_of[8], (LAYERS, D, FF), D ** -0.5, 0.21875, ((0, 2),)),
        "down_weight": scatter_about(streams_of[9], (LAYERS, FF, D), FF ** -0.5, 0.109375, ((0, 2),)),
        "key_pool": scatter_about(streams_of[10], (LAYERS, KERNEL, D), 0.45, 2.5, ((0, 2),), jnp.float32),
        "value_pool": scatter_about(streams_of[11], (LAYERS, KERNEL, D), 0.45, 2.5, ((0, 2),), jnp.float32),
        "attn_norm_gain": jnp.clip(1.0 + 0.1 * jax.random.normal(streams_of[12], (LAYERS, D), jnp.float32), 0.5, 1.5),
        "attn_norm_bias": scatter_about(streams_of[13], (LAYERS, D), 0.5, 3.0, ((0, 2),), jnp.float32),
        "ffn_norm_gain": jnp.clip(1.0 + 0.1 * jax.random.normal(streams_of[14], (LAYERS, D), jnp.float32), 0.5, 1.5),
        "ffn_norm_bias": scatter_about(streams_of[15], (LAYERS, D), 0.5, 3.0, ((0, 2),), jnp.float32),
    }


highest = lax.Precision.HIGHEST
epsilon = 1e-05
masked_score = -1e+30

@jax.custom_vjp
def low(v):
    return lax.optimization_barrier(v.astype(jnp.bfloat16)).astype(jnp.float32)

@jax.custom_vjp
def low_back(v):
    return v

def low_keep(v):
    return (low(v), None)

def low_pass(kept, grad):
    return (grad,)

def back_keep(v):
    return (v, None)

def back_low(kept, grad):
    return (low(grad),)
low.defvjp(low_keep, low_pass)
low_back.defvjp(back_keep, back_low)

def both_ways(value):
    return low(low_back(value))

def norm_rows(state, gain, shift):
    average = lax.optimization_barrier(jnp.mean(state, axis=-1, keepdims=True))
    centred = state - average
    variance = lax.optimization_barrier(jnp.mean(centred * centred, axis=-1, keepdims=True))
    return centred * lax.rsqrt(variance + epsilon) * gain + shift

def pool_taps(extended, taps, rows, offset):
    centre = taps.shape[0] // 2
    total = None
    for tap in range(taps.shape[0]):
        begin = offset + tap - centre
        slab = lax.slice_in_dim(extended, begin, begin + rows, axis=0)
        slab = slab.reshape(rows // STRIDE, STRIDE, slab.shape[1])[:, 0]
        term = taps[tap] * slab
        total = term if total is None else total + term
    return total

def key_mask(row_pos, raw_first, pool_first, raw_count, pool_count, length, valid):
    half = WIN // 2
    reach = PWIN // 2
    raw_pos = raw_first + jnp.arange(raw_count, dtype=jnp.int32)
    raw_valid = (raw_pos >= 0) & (raw_pos < length)
    raw_valid = raw_valid[None, :] & (raw_pos[None, :] >= row_pos[:, None] - half) & (raw_pos[None, :] < row_pos[:, None] + half)
    pool_index = pool_first + jnp.arange(pool_count, dtype=jnp.int32)
    pool_valid = (pool_index >= 0) & (pool_index < length // STRIDE)
    pool_valid = pool_valid[None, :] & (STRIDE * pool_index[None, :] >= row_pos[:, None] - reach) & (STRIDE * pool_index[None, :] < row_pos[:, None] + reach)
    question_valid = jnp.broadcast_to(valid[None, :], (row_pos.shape[0], valid.shape[0]))
    return jnp.concatenate([raw_valid, pool_valid, question_valid], axis=1)

def attend(rows_query, keys, values, mask):
    count = rows_query.shape[0]
    width = rows_query.shape[1]
    heads = width // DH
    scale = 1.0 / math.sqrt(DH)
    score = jnp.einsum('thd,khd->htk', rows_query.reshape(count, heads, DH), keys.reshape(-1, heads, DH), precision=highest) * scale
    score = low_back(score)
    score = jnp.where(mask[None], score, masked_score)
    top = lax.optimization_barrier(jnp.max(score, axis=-1, keepdims=True))
    weights = jnp.exp(score - top)
    softened = low(weights / lax.optimization_barrier(jnp.sum(weights, axis=-1, keepdims=True)))
    result = jnp.einsum('htk,khd->thd', softened, values.reshape(-1, heads, DH), precision=highest)
    return result.reshape(count, width)

def layer(state, params, positions, count):
    query_w, key_w, value_w, output_w, up_w, down_w, key_taps, value_taps, gain_one, bias_one, gain_two, bias_two = params
    length = state.shape[0]
    width = state.shape[1]
    half = WIN // 2
    pool_half = PWIN // (2 * STRIDE)
    centre = KERNEL // 2
    normed = low(norm_rows(state, gain_one, bias_one))
    query = both_ways(jnp.dot(normed, query_w, precision=highest))
    keys = both_ways(jnp.dot(normed, key_w, precision=highest))
    values = both_ways(jnp.dot(normed, value_w, precision=highest))
    pair = jnp.concatenate([keys, values], axis=1)
    padded = jnp.pad(pair, ((centre, centre), (0, 0)))
    taps = jnp.concatenate([key_taps, value_taps], axis=1)
    pooled = both_ways(pool_taps(padded, taps, length, centre))
    pooled_keys = pooled[:, :width]
    pooled_values = pooled[:, width:]
    slots = jnp.arange(QMAX, dtype=jnp.int32)
    valid = slots < count
    question_q = jnp.take(query, positions, axis=0)
    question_k = jnp.take(keys, positions, axis=0)
    question_v = jnp.take(values, positions, axis=0)
    key_window = jnp.pad(keys, ((half, half), (0, 0)))
    value_window = jnp.pad(values, ((half, half), (0, 0)))
    pool_key_window = jnp.pad(pooled_keys, ((pool_half, pool_half), (0, 0)))
    pool_value_window = jnp.pad(pooled_values, ((pool_half, pool_half), (0, 0)))
    block = math.gcd(length, 512)

    def block_out(start):
        raw_keys = lax.dynamic_slice_in_dim(key_window, start, block + 2 * half)
        raw_values = lax.dynamic_slice_in_dim(value_window, start, block + 2 * half)
        pool_start = start // STRIDE
        pool_keys = lax.dynamic_slice_in_dim(pool_key_window, pool_start, block // STRIDE + 2 * pool_half)
        pool_values = lax.dynamic_slice_in_dim(pool_value_window, pool_start, block // STRIDE + 2 * pool_half)
        row_pos = start + jnp.arange(block, dtype=jnp.int32)
        mask = key_mask(row_pos, start - half, pool_start - pool_half, block + 2 * half, block // STRIDE + 2 * pool_half, length, valid)
        rows_query = lax.dynamic_slice_in_dim(query, start, block)
        all_keys = jnp.concatenate([raw_keys, pool_keys, question_k], axis=0)
        all_values = jnp.concatenate([raw_values, pool_values, question_v], axis=0)
        return attend(rows_query, all_keys, all_values, mask)
    starts = jnp.arange(length // block, dtype=jnp.int32) * block
    local = lax.map(jax.checkpoint(block_out), starts).reshape(length, width)
    question_out = attend(question_q, keys, values, jnp.ones((QMAX, length), dtype=bool))
    onehot = ((positions[:, None] == jnp.arange(length, dtype=jnp.int32)[None, :]) & valid[:, None]).astype(jnp.float32)
    is_question = lax.optimization_barrier(jnp.sum(onehot, axis=0)) > 0
    replaced = jnp.dot(onehot.T, question_out, precision=highest)
    mixed = both_ways(jnp.where(is_question[:, None], replaced, local))
    middle = state + low_back(jnp.dot(mixed, output_w, precision=highest))
    normed_two = low(norm_rows(middle, gain_two, bias_two))
    hidden = low_back(jnp.dot(normed_two, up_w, precision=highest))
    active = low(jax.nn.gelu(hidden, approximate=False))
    return middle + low_back(jnp.dot(active, down_w, precision=highest))

def reference(inputs, cotangent, question_positions, question_counts, query_weight, key_weight, value_weight, output_weight, up_weight, down_weight, key_pool, value_pool, attn_norm_gain, attn_norm_bias, ffn_norm_gain, ffn_norm_bias):
    weights = tuple((array.astype(jnp.float32) for array in (query_weight, key_weight, value_weight, output_weight, up_weight, down_weight, key_pool, value_pool, attn_norm_gain, attn_norm_bias, ffn_norm_gain, ffn_norm_bias)))

    def one_item(carry, item):
        state, grad_out, positions, count = item
        state = state.astype(jnp.float32)

        def forward(start_state, probe, params):
            first = tuple((array[0] for array in params))
            second = tuple((array[1] for array in params))
            middle = layer(start_state, first, positions, count)
            passed = low(low_back(middle + probe))
            final = layer(passed, second, positions, count)
            return (passed, final)
        (passed, final), pullback = jax.vjp(forward, state, jnp.zeros_like(state), weights)
        grad_state, grad_probe, grad_params = pullback((jnp.zeros_like(passed), grad_out.astype(jnp.float32)))
        carry = tuple((total + part for total, part in zip(carry, grad_params)))
        return (carry, (passed.astype(jnp.bfloat16), final.astype(jnp.bfloat16), grad_state.astype(jnp.bfloat16), grad_probe.astype(jnp.bfloat16)))
    init = tuple((jnp.zeros_like(array) for array in weights))
    totals, (passed, final, grad_state, grad_probe) = lax.scan(one_item, init, (inputs, cotangent, question_positions, question_counts))
    section_outputs = jnp.stack([passed, final])
    input_grads = jnp.stack([grad_state, grad_probe])
    return (section_outputs, input_grads, totals[0], totals[1], totals[2], totals[3], totals[4], totals[5], totals[6], totals[7], totals[8], totals[9], totals[10], totals[11])
```

```python
import math

import jax
import jax.numpy as jnp
from jax import lax
from jax.sharding import PartitionSpec as P

DH = 64
WIN = 128
PWIN = 512
STRIDE = 4
QMAX = 64


epsilon = 1e-05
highest = lax.Precision.HIGHEST
masked_score = -1e30


def padded(shard, sides, width):
    for axis, dim in sides:
        devices, length = (lax.axis_size(axis), shard.shape[dim])
        up = [(i, (i + 1) % devices) for i in range(devices - 1)]
        down = [(j, i) for i, j in up]
        last = lax.slice_in_dim(shard, length - width, length, axis=dim)
        first = lax.slice_in_dim(shard, 0, width, axis=dim)
        before = lax.ppermute(last, axis, up)
        after = lax.ppermute(first, axis, down)
        shard = jnp.concatenate([before, shard, after], axis=dim)
    return shard


def merged(shard, axis, combine):
    everything = jax.tree.map(lambda part: lax.all_gather(part, axis), shard)
    first = jax.tree.map(lambda part: part[0], everything)

    def lap(k, so_far):
        return combine(so_far, jax.tree.map(lambda part: part[k], everything))

    return lax.fori_loop(1, lax.axis_size(axis), lap, first)


def swapped(block, axis, apart):
    count = lax.axis_size(axis)
    route = []
    for low in range(count):
        high = low | 1 << apart
        if high != low and high < count:
            route += [(low, high), (high, low)]
    return lax.ppermute(block, axis, route)


def norm_rows(state, gain, shift):
    average = jnp.mean(state, axis=-1, keepdims=True)
    centred = state - average
    variance = jnp.mean(centred * centred, axis=-1, keepdims=True)
    return centred * lax.rsqrt(variance + epsilon) * gain + shift


def gelu_exact(value):
    return jax.nn.gelu(value, approximate=False)


def pool_taps(extended, taps, rows, offset):
    centre = taps.shape[0] // 2
    total = None
    for tap in range(taps.shape[0]):
        begin = offset + tap - centre
        slab = lax.slice_in_dim(extended, begin, begin + rows, axis=0)
        slab = slab.reshape(rows // STRIDE, STRIDE, slab.shape[1])[:, 0]
        term = taps[tap] * slab
        total = term if total is None else total + term
    return total


def key_mask(row_pos, raw_first, pool_first, raw_count, pool_count, length, valid):
    half = WIN // 2
    reach = PWIN // 2
    raw_pos = raw_first + jnp.arange(raw_count, dtype=jnp.int32)
    raw_valid = (raw_pos >= 0) & (raw_pos < length)
    raw_valid = (
        raw_valid[None, :]
        & (raw_pos[None, :] >= row_pos[:, None] - half)
        & (raw_pos[None, :] < row_pos[:, None] + half)
    )
    pool_index = pool_first + jnp.arange(pool_count, dtype=jnp.int32)
    pool_valid = (pool_index >= 0) & (pool_index < length // STRIDE)
    pool_valid = (
        pool_valid[None, :]
        & (STRIDE * pool_index[None, :] >= row_pos[:, None] - reach)
        & (STRIDE * pool_index[None, :] < row_pos[:, None] + reach)
    )
    question_valid = jnp.broadcast_to(valid[None, :], (row_pos.shape[0], valid.shape[0]))
    return jnp.concatenate([raw_valid, pool_valid, question_valid], axis=1)


def inner_rows(left, right):
    return lax.dot_general(
        left, right, (((0,), (0,)), ((), ())), preferred_element_type=jnp.float32
    )


def times_transposed(left, right):
    return lax.dot_general(
        left, right, (((1,), (1,)), ((), ())), preferred_element_type=jnp.float32
    )


def merge_stats(first, second):
    top = jnp.maximum(first[0], second[0])
    total = first[1] * jnp.exp(first[0] - top) + second[1] * jnp.exp(second[0] - top)
    return (top, total)


def return_rims(grads, width):
    edges = jnp.concatenate([grads[:width], grads[-width:]], axis=0)
    arrived = padded(edges.astype(jnp.bfloat16), (("seq", 0),), width).astype(edges.dtype)
    inner = grads[width:-width]
    count = inner.shape[0]
    inner = inner + jnp.pad(arrived[:width], ((0, count - width), (0, 0)))
    return inner + jnp.pad(arrived[3 * width :], ((count - width, 0), (0, 0)))


def return_pooled(grads, width):
    edges = jnp.concatenate([grads[:width], grads[-width:]], axis=0)
    arrived = padded(edges.astype(jnp.bfloat16), (("seq", 0),), width).astype(edges.dtype)
    inner = grads[width:-width]
    inner = inner + arrived[:width]
    return inner + arrived[3 * width :]


def layer_forward(state, params, positions, count):
    rows = state.shape[0]
    width = state.shape[1]
    heads = width // DH
    scale = 1.0 / math.sqrt(DH)
    half = WIN // 2
    pool_half = PWIN // (2 * STRIDE)
    base = lax.axis_index("seq") * rows
    length = lax.axis_size("seq") * rows
    normed = norm_rows(state, params["gain_one"], params["bias_one"]).astype(jnp.bfloat16)
    query = jnp.dot(normed, params["query"], preferred_element_type=jnp.float32).astype(
        jnp.bfloat16
    )
    keys = jnp.dot(normed, params["key"], preferred_element_type=jnp.float32).astype(jnp.bfloat16)
    values = jnp.dot(normed, params["value"], preferred_element_type=jnp.float32).astype(
        jnp.bfloat16
    )
    pair = jnp.concatenate([keys, values], axis=1)
    extended = padded(pair, (("seq", 0),), half)
    taps = jnp.concatenate([params["key_pool"], params["value_pool"]], axis=1)
    pooled = pool_taps(extended.astype(jnp.float32), taps, rows, half).astype(jnp.bfloat16)
    pooled_ext = padded(pooled, (("seq", 0),), pool_half)
    slots = jnp.arange(QMAX, dtype=jnp.int32)
    valid = slots < count
    row_pos = base + jnp.arange(rows, dtype=jnp.int32)
    select = (positions[:, None] == row_pos[None, :]) & valid[:, None]
    select_low = select.astype(jnp.bfloat16)
    select_float = select.astype(jnp.float32)
    triple = jnp.concatenate([query, keys, values], axis=1)
    picked = jnp.dot(select_low, triple, preferred_element_type=jnp.float32)
    picked = lax.psum(picked.astype(jnp.bfloat16), "seq")
    question_q = picked[:, :width]
    question_k = picked[:, width : 2 * width]
    question_v = picked[:, 2 * width :]
    all_keys = jnp.concatenate([extended[:, :width], pooled_ext[:, :width], question_k], axis=0)
    all_values = jnp.concatenate([extended[:, width:], pooled_ext[:, width:], question_v], axis=0)
    mask = key_mask(
        row_pos,
        base - half,
        base // STRIDE - pool_half,
        rows + 2 * half,
        rows // STRIDE + 2 * pool_half,
        length,
        valid,
    )
    query3 = query.reshape(rows, heads, DH)
    keys3 = all_keys.reshape(-1, heads, DH)
    values3 = all_values.reshape(-1, heads, DH)
    score = jnp.einsum("thd,khd->htk", query3, keys3, preferred_element_type=jnp.float32) * scale
    score = jnp.where(mask[None], score, masked_score)
    top = jnp.max(score, axis=-1, keepdims=True)
    weights = jnp.exp(score - top)
    softened = weights / jnp.sum(weights, axis=-1, keepdims=True)
    softened_low = softened.astype(jnp.bfloat16)
    local_out = jnp.einsum(
        "htk,khd->thd", softened_low, values3, preferred_element_type=jnp.float32
    ).reshape(rows, width)
    own_keys3 = keys.reshape(rows, heads, DH)
    own_values3 = values.reshape(rows, heads, DH)
    question3 = question_q.reshape(QMAX, heads, DH)
    question_score = (
        jnp.einsum("chd,thd->hct", question3, own_keys3, preferred_element_type=jnp.float32) * scale
    )
    question_top = jnp.max(question_score, axis=-1, keepdims=True)
    question_total = jnp.sum(jnp.exp(question_score - question_top), axis=-1, keepdims=True)
    global_top, global_total = merged((question_top, question_total), "seq", merge_stats)
    log_total = global_top + jnp.log(global_total)
    question_soft = jnp.exp(question_score - log_total)
    question_soft_low = question_soft.astype(jnp.bfloat16)
    numerator = jnp.einsum(
        "hct,thd->chd", question_soft_low, own_values3, preferred_element_type=jnp.float32
    )
    exact = jnp.einsum(
        "hct,thd->chd", question_soft, own_values3.astype(jnp.float32), precision=highest
    )
    numerator, exact = (
        lax.psum(numerator.astype(jnp.bfloat16), "seq").astype(jnp.float32),
        lax.psum(exact.astype(jnp.bfloat16), "seq").astype(jnp.float32),
    )
    is_question = jnp.sum(select_float, axis=0) > 0
    replaced = jnp.dot(select_float.T, numerator.reshape(QMAX, width), precision=highest)
    mixed_low = jnp.where(is_question[:, None], replaced, local_out).astype(jnp.bfloat16)
    middle = state + jnp.dot(mixed_low, params["output"], preferred_element_type=jnp.float32)
    normed_two = norm_rows(middle, params["gain_two"], params["bias_two"]).astype(jnp.bfloat16)
    hidden = jnp.dot(normed_two, params["up"], preferred_element_type=jnp.float32)
    active = gelu_exact(hidden).astype(jnp.bfloat16)
    result = middle + jnp.dot(active, params["down"], preferred_element_type=jnp.float32)
    tape = {
        "normed": normed,
        "query3": query3,
        "extended": extended,
        "taps": taps,
        "select_low": select_low,
        "select_float": select_float,
        "is_question": is_question,
        "keys3": keys3,
        "values3": values3,
        "softened": softened,
        "softened_low": softened_low,
        "question3": question3,
        "own_keys3": own_keys3,
        "own_values3": own_values3,
        "question_soft": question_soft,
        "question_soft_low": question_soft_low,
        "exact": exact,
        "mixed_low": mixed_low,
        "middle": middle,
        "normed_two": normed_two,
        "hidden": hidden,
        "active": active,
    }
    return (result, tape)


def layer_backward(state, grad_out, params, tape):
    rows = state.shape[0]
    width = state.shape[1]
    heads = width // DH
    scale = 1.0 / math.sqrt(DH)
    half = WIN // 2
    pool_half = PWIN // (2 * STRIDE)
    grads = {}
    grad_low = grad_out.astype(jnp.bfloat16)
    grads["down"] = inner_rows(tape["active"], grad_low)
    grad_active = times_transposed(grad_low, params["down"])
    _, gelu_back = jax.vjp(gelu_exact, tape["hidden"])
    grad_hidden = gelu_back(grad_active)[0].astype(jnp.bfloat16)
    grads["up"] = inner_rows(tape["normed_two"], grad_hidden)
    grad_normed_two = times_transposed(grad_hidden, params["up"])
    _, norm_back_two = jax.vjp(norm_rows, tape["middle"], params["gain_two"], params["bias_two"])
    grad_middle, grads["gain_two"], grads["bias_two"] = norm_back_two(grad_normed_two)
    grad_middle = grad_middle + grad_out
    branch_low = grad_middle.astype(jnp.bfloat16)
    grads["output"] = inner_rows(tape["mixed_low"], branch_low)
    grad_mixed = times_transposed(branch_low, params["output"]).astype(jnp.bfloat16)
    grad_question_out = jnp.dot(tape["select_low"], grad_mixed, preferred_element_type=jnp.float32)
    grad_question_out = lax.psum(grad_question_out.astype(jnp.bfloat16), "seq")
    grad_local = jnp.where(tape["is_question"][:, None], jnp.zeros_like(grad_mixed), grad_mixed)
    grad_local3 = grad_local.reshape(rows, heads, DH)
    softened = tape["softened"]
    grad_soft = jnp.einsum(
        "thd,khd->htk", grad_local3, tape["values3"], preferred_element_type=jnp.float32
    )
    delta = jnp.sum(softened * grad_soft, axis=-1, keepdims=True)
    grad_score = (softened * (grad_soft - delta)).astype(jnp.bfloat16)
    grad_query = (
        jnp.einsum(
            "htk,khd->thd", grad_score, tape["keys3"], preferred_element_type=jnp.float32
        ).reshape(rows, width)
        * scale
    )
    grad_keys_all = (
        jnp.einsum(
            "htk,thd->khd", grad_score, tape["query3"], preferred_element_type=jnp.float32
        ).reshape(-1, width)
        * scale
    )
    grad_values_all = jnp.einsum(
        "htk,thd->khd", tape["softened_low"], grad_local3, preferred_element_type=jnp.float32
    ).reshape(-1, width)
    question_grad3 = grad_question_out.reshape(QMAX, heads, DH)
    question_soft = tape["question_soft"]
    question_grad_soft = jnp.einsum(
        "chd,thd->hct", question_grad3, tape["own_values3"], preferred_element_type=jnp.float32
    )
    question_delta = jnp.sum(question_grad3.astype(jnp.float32) * tape["exact"], axis=-1).T[
        :, :, None
    ]
    question_grad_score = (question_soft * (question_grad_soft - question_delta)).astype(
        jnp.bfloat16
    )
    grad_question_q = (
        jnp.einsum(
            "hct,thd->chd",
            question_grad_score,
            tape["own_keys3"],
            preferred_element_type=jnp.float32,
        ).reshape(QMAX, width)
        * scale
    )
    grad_own_keys = (
        jnp.einsum(
            "hct,chd->thd",
            question_grad_score,
            tape["question3"],
            preferred_element_type=jnp.float32,
        ).reshape(rows, width)
        * scale
    )
    grad_own_values = jnp.einsum(
        "hct,chd->thd",
        tape["question_soft_low"],
        question_grad3,
        preferred_element_type=jnp.float32,
    ).reshape(rows, width)
    raw_count = rows + 2 * half
    pool_count = rows // STRIDE + 2 * pool_half
    grad_raw = jnp.concatenate([grad_keys_all[:raw_count], grad_values_all[:raw_count]], axis=1)
    grad_pool = jnp.concatenate(
        [
            grad_keys_all[raw_count : raw_count + pool_count],
            grad_values_all[raw_count : raw_count + pool_count],
        ],
        axis=1,
    )
    grad_question_k = grad_keys_all[raw_count + pool_count :]
    grad_question_v = grad_values_all[raw_count + pool_count :]
    sent_q, sent_k, sent_v = (
        lax.psum(grad_question_q.astype(jnp.bfloat16), "seq").astype(jnp.float32),
        lax.psum(grad_question_k.astype(jnp.bfloat16), "seq").astype(jnp.float32),
        lax.psum(grad_question_v.astype(jnp.bfloat16), "seq").astype(jnp.float32),
    )
    own_pool = return_pooled(grad_pool, pool_half)
    pool_low = own_pool.astype(jnp.bfloat16).astype(jnp.float32)

    def pool_piece(extended_values, taps_values):
        return pool_taps(extended_values, taps_values, rows, half)

    _, pool_back = jax.vjp(pool_piece, tape["extended"].astype(jnp.float32), tape["taps"])
    grad_extended, grad_taps = pool_back(pool_low)
    own_raw = return_rims(grad_raw + grad_extended, half)
    select_t = tape["select_float"].T
    own_raw = own_raw + jnp.concatenate([grad_own_keys, grad_own_values], axis=1)
    own_raw = own_raw + jnp.dot(
        select_t, jnp.concatenate([sent_k, sent_v], axis=1), precision=highest
    )
    grad_query = grad_query + jnp.dot(select_t, sent_q, precision=highest)
    query_low = grad_query.astype(jnp.bfloat16)
    key_low = own_raw[:, :width].astype(jnp.bfloat16)
    value_low = own_raw[:, width:].astype(jnp.bfloat16)
    grads["query"] = inner_rows(tape["normed"], query_low)
    grads["key"] = inner_rows(tape["normed"], key_low)
    grads["value"] = inner_rows(tape["normed"], value_low)
    grad_normed = (
        times_transposed(query_low, params["query"])
        + times_transposed(key_low, params["key"])
        + times_transposed(value_low, params["value"])
    )
    _, norm_back_one = jax.vjp(norm_rows, state, params["gain_one"], params["bias_one"])
    grad_state, grads["gain_one"], grads["bias_one"] = norm_back_one(grad_normed)
    grads["key_pool"] = grad_taps[:, :width]
    grads["value_pool"] = grad_taps[:, width:]
    return (grad_state + grad_middle, grads)


def to_partner(block):
    return swapped(block, "section", 0)


def per_device(
    inputs,
    cotangent,
    question_positions,
    question_counts,
    query_weight,
    key_weight,
    value_weight,
    output_weight,
    up_weight,
    down_weight,
    key_pool,
    value_pool,
    attn_norm_gain,
    attn_norm_bias,
    ffn_norm_gain,
    ffn_norm_bias,
):
    names = (
        "query",
        "key",
        "value",
        "output",
        "up",
        "down",
        "key_pool",
        "value_pool",
        "gain_one",
        "bias_one",
        "gain_two",
        "bias_two",
    )
    arrays = (
        query_weight,
        key_weight,
        value_weight,
        output_weight,
        up_weight,
        down_weight,
        key_pool,
        value_pool,
        attn_norm_gain,
        attn_norm_bias,
        ffn_norm_gain,
        ffn_norm_bias,
    )
    params = {name: array[0] for name, array in zip(names, arrays)}
    section = lax.axis_index("section")
    micro = inputs.shape[0]
    rows = inputs.shape[1]
    width = inputs.shape[2]
    received = jnp.zeros((rows, width), jnp.bfloat16)
    states = []
    tapes = []
    made = []
    for tick in range(micro + 1):
        slot = jnp.clip(tick - section, 0, micro - 1)
        layer_in = jnp.where(section == 0, inputs[min(tick, micro - 1)], received)
        state = layer_in.astype(jnp.float32)
        result, tape = layer_forward(
            state, params, question_positions[slot], question_counts[slot]
        )
        result_low = result.astype(jnp.bfloat16)
        states.append(state)
        tapes.append(tape)
        made.append(result_low)
        if tick < micro:
            received = to_partner(result_low)
    produced = jnp.where(section == 0, jnp.stack(made[:micro]), jnp.stack(made[1:]))
    totals = {name: jnp.zeros(params[name].shape, jnp.float32) for name in names}
    grad_in = jnp.zeros((rows, width), jnp.bfloat16)
    back = []
    for tick in range(micro + 1):
        first = tick + section >= 1
        last = tick + section <= micro
        factor = (first & last).astype(jnp.float32)
        grad_out = jnp.where(section == 1, cotangent[max(micro - 1 - tick, 0)], grad_in)
        grad_state, grads = layer_backward(
            states[micro - tick], grad_out.astype(jnp.float32), params, tapes[micro - tick]
        )
        totals = {name: totals[name] + factor * grads[name] for name in names}
        grad_state_low = grad_state.astype(jnp.bfloat16)
        back.append(grad_state_low)
        if tick < micro:
            grad_in = to_partner(grad_state_low)
    back_grads = jnp.where(
        section == 0, jnp.stack(back[1:][::-1]), jnp.stack(back[:micro][::-1])
    )
    flat = tuple((totals[name].reshape(-1, totals[name].shape[-1]) for name in names))
    summed = lax.psum(tuple(part.astype(jnp.bfloat16) for part in flat), ("dp", "seq"))
    summed = tuple(part.astype(jnp.float32) for part in summed)
    outs = tuple((part.reshape((1,) + params[name].shape) for part, name in zip(summed, names)))
    return (
        produced[None],
        back_grads[None],
        outs[0],
        outs[1],
        outs[2],
        outs[3],
        outs[4],
        outs[5],
        outs[6],
        outs[7],
        outs[8],
        outs[9],
        outs[10],
        outs[11],
    )


def solution(mesh):
    in_specs = (
        P("dp", "seq", None),
        P("dp", "seq", None),
        P("dp", None),
        P("dp"),
        P("section", None, None),
        P("section", None, None),
        P("section", None, None),
        P("section", None, None),
        P("section", None, None),
        P("section", None, None),
        P("section", None, None),
        P("section", None, None),
        P("section", None),
        P("section", None),
        P("section", None),
        P("section", None),
    )
    out_specs = (
        P("section", "dp", "seq", None),
        P("section", "dp", "seq", None),
        P("section", None, None),
        P("section", None, None),
        P("section", None, None),
        P("section", None, None),
        P("section", None, None),
        P("section", None, None),
        P("section", None, None),
        P("section", None, None),
        P("section", None),
        P("section", None),
        P("section", None),
        P("section", None),
    )
    return jax.shard_map(
        per_device, mesh=mesh, in_specs=in_specs, out_specs=out_specs, check_vma=False
    )
```

```python
import functools
import math

import jax
import jax.numpy as jnp
from jax import lax
from jax.experimental import pallas as pl
from jax.experimental.pallas import tpu as pltpu
from jax.sharding import PartitionSpec as P

DH = 64
WIN = 128
PWIN = 512
STRIDE = 4
QMAX = 64
TAIL = 16
LANES = 128

epsilon = 1e-05
masked_score = -1e30
scale = 1.0 / math.sqrt(DH)
half = WIN // 2
pool_half = PWIN // (2 * STRIDE)
low = jnp.bfloat16
full = jnp.float32
SECTION, DP, SEQ = "section", "dp", "seq"
MESH = pl.DeviceIdType.MESH


def norm_rows(state, gain, shift):
    average = jnp.mean(state, axis=-1, keepdims=True)
    centred = state - average
    variance = jnp.mean(centred * centred, axis=-1, keepdims=True)
    return centred * lax.rsqrt(variance + epsilon) * gain + shift


def gelu_parts(value):
    spread = 0.5 + 0.5 * lax.erf(value * math.sqrt(0.5))
    slope = spread + value * jnp.exp(-0.5 * value * value) * (1.0 / math.sqrt(2.0 * math.pi))
    return (value * spread).astype(low), slope.astype(low)


def mm(left, right):
    return jnp.dot(left, right, preferred_element_type=full)


def tn(left, right):
    return lax.dot_general(left, right, (((0,), (0,)), ((), ())), preferred_element_type=full)


def nt(left, right):
    return lax.dot_general(left, right, (((1,), (1,)), ((), ())), preferred_element_type=full)


def exchange_kernel(count, plan, live, reduce, n_in, n_out, *refs):
    ins, outs = refs[:n_in], refs[n_in : n_in + n_out]
    send_sem, recv_sem, keep_sem = refs[n_in + n_out : n_in + n_out + 3]
    slots = refs[n_in + n_out + 3 :]
    me = lax.axis_index(SEQ)

    def run():
        barrier = pltpu.get_barrier_semaphore()
        for step in range(1, count):
            peer = lax.rem(me + step, count)
            pl.semaphore_signal(barrier, inc=1, device_id={SEQ: peer}, device_id_type=MESH)
        pl.semaphore_wait(barrier, count - 1)
        jobs = []
        sem = 0
        for src, first, rows, shift, dst, at in plan:
            if shift is None:
                buffer = slots[dst]
                for step in range(1, count):
                    peer = lax.rem(me + step, count)
                    copy = pltpu.make_async_remote_copy(
                        src_ref=ins[src].at[pl.ds(first, rows)],
                        dst_ref=buffer.at[step - 1],
                        send_sem=send_sem.at[sem],
                        recv_sem=recv_sem.at[sem],
                        device_id={SEQ: peer},
                        device_id_type=MESH,
                    )
                    copy.start()
                    jobs.append((copy, None, None))
                    sem += 1
            else:
                target, source = me + shift, me - shift
                can_send = (target >= 0) & (target < count)
                can_take = (source >= 0) & (source < count)
                copy = pltpu.make_async_remote_copy(
                    src_ref=ins[src].at[pl.ds(first, rows)],
                    dst_ref=outs[dst].at[pl.ds(at, rows)],
                    send_sem=send_sem.at[sem],
                    recv_sem=recv_sem.at[sem],
                    device_id={SEQ: jnp.clip(target, 0, count - 1)},
                    device_id_type=MESH,
                )

                @pl.when(can_send)
                def _():
                    copy.start()

                @pl.when(jnp.logical_not(can_take))
                def _():
                    outs[dst][pl.ds(at, rows), :] = jnp.zeros((rows, outs[dst].shape[1]), outs[dst].dtype)

                jobs.append((copy, can_send, can_take))
                sem += 1
        for copy, can_send, can_take in jobs:
            if can_send is None:
                copy.wait_send()
                copy.wait_recv()
            else:
                pl.when(can_send)(copy.wait_send)
                pl.when(can_take)(copy.wait_recv)

    if live is None:
        run()
    else:
        on = lax.axis_index(SECTION) == live
        pl.when(on)(run)

        @pl.when(jnp.logical_not(on))
        def _():
            for out in outs:
                out[...] = jnp.zeros(out.shape, out.dtype)
            for buffer in slots:
                buffer[...] = jnp.zeros(buffer.shape, buffer.dtype)

    reduce(ins, outs, slots)


def exchange(ident, live, inputs, plan, out_shapes, slot_shapes, reduce):
    count = lax.axis_size(SEQ)
    copies = sum(count - 1 if item[3] is None else 1 for item in plan)
    vmem = pl.BlockSpec(memory_space=pltpu.VMEM)
    kernel = functools.partial(
        exchange_kernel, count, plan, live, reduce, len(inputs), len(out_shapes)
    )
    return pl.pallas_call(
        kernel,
        out_shape=[jax.ShapeDtypeStruct(s, t) for s, t in out_shapes],
        in_specs=[vmem] * len(inputs),
        out_specs=[vmem] * len(out_shapes),
        scratch_shapes=[
            pltpu.SemaphoreType.DMA((copies,)),
            pltpu.SemaphoreType.DMA((copies,)),
            pltpu.SemaphoreType.DMA((1,)),
        ]
        + [pltpu.VMEM((count - 1,) + s, t) for s, t in slot_shapes],
        compiler_params=pltpu.CompilerParams(collective_id=ident, has_side_effects=True),
    )(*inputs)


def slot_sum(own, slots):
    total = own.astype(full)
    for k in range(slots.shape[0]):
        total = total + slots[k].astype(full)
    return total


def gather_rows(ident, live, state, pick):
    rows, width = state.shape
    own = TAIL + rows
    right = own + rows
    quest = right + rows
    plan = (
        (1, 0, QMAX, None, 0, 0),
        (0, rows - TAIL, TAIL, 2, 0, 0),
        (0, 0, rows, -1, 0, right),
        (0, 0, rows, 1, 0, TAIL),
    )

    def reduce(ins, outs, slots):
        outs[0][pl.ds(own, rows), :] = ins[0][...]
        outs[0][pl.ds(quest, QMAX), :] = slot_sum(ins[1][...], slots[0]).astype(low)

    return exchange(
        ident,
        live,
        (state, pick),
        plan,
        (((quest + QMAX, width), low),),
        (((QMAX, width), low),),
        reduce,
    )[0]


def return_rows(ident, live, grads, rows):
    width = grads.shape[1]
    own = TAIL + rows
    right = own + rows
    quest = right + rows
    plan = (
        (0, quest, QMAX, None, 0, 0),
        (0, 0, TAIL, -2, 4, 0),
        (0, TAIL, rows, -1, 2, 0),
        (0, right, rows, 1, 3, 0),
    )

    def reduce(ins, outs, slots):
        total = ins[0][pl.ds(own, rows), :].astype(full)
        total = total + outs[2][...].astype(full) + outs[3][...].astype(full)
        outs[0][...] = total
        outs[0][pl.ds(rows - TAIL, TAIL), :] += outs[4][...].astype(full)
        outs[1][...] = slot_sum(ins[0][pl.ds(quest, QMAX), :], slots[0])

    return exchange(
        ident,
        live,
        (grads,),
        plan,
        (
            ((rows, width), full),
            ((QMAX, width), full),
            ((rows, width), low),
            ((rows, width), low),
            ((TAIL, width), low),
        ),
        (((QMAX, width), low),),
        reduce,
    )[:2]


def broadcast(count, pieces, send_sem, recv_sem):
    me = lax.axis_index(SEQ)
    copies = []
    for k, (src, slots) in enumerate(pieces):
        for step in range(1, count):
            index = k * (count - 1) + step - 1
            copies.append(
                pltpu.make_async_remote_copy(
                    src_ref=src,
                    dst_ref=slots.at[step - 1],
                    send_sem=send_sem.at[index],
                    recv_sem=recv_sem.at[index],
                    device_id={SEQ: lax.rem(me + step, count)},
                    device_id_type=MESH,
                )
            )
    return copies


def greet(count):
    me = lax.axis_index(SEQ)
    barrier = pltpu.get_barrier_semaphore()
    for step in range(1, count):
        peer = lax.rem(me + step, count)
        pl.semaphore_signal(barrier, inc=1, device_id={SEQ: peer}, device_id_type=MESH)
    pl.semaphore_wait(barrier, count - 1)


def when_live(live, action):
    if live is None:
        action()
    else:
        pl.when(lax.axis_index(SECTION) == live)(action)


def begin_all(count, live, pieces, send_sem, recv_sem):
    def start():
        greet(count)
        for copy in broadcast(count, pieces, send_sem, recv_sem):
            copy.start()

    when_live(live, start)


def finish_all(count, live, pieces, send_sem, recv_sem):
    def finish():
        for copy in broadcast(count, pieces, send_sem, recv_sem):
            copy.wait()

    when_live(live, finish)
    if live is not None:

        @pl.when(lax.axis_index(SECTION) != live)
        def _():
            for _, slots in pieces:
                slots[...] = jnp.zeros(slots.shape, slots.dtype)


def merge_questions(numerator, stats, numerators, many, answer, merged):
    tops = [stats[...]] + [many[k] for k in range(many.shape[0])]
    parts = [numerator] + [numerators.at[k] for k in range(numerators.shape[0])]
    merged[...] = jnp.zeros_like(merged)
    for p in range(numerator.shape[1] // LANES):
        top = tops[0][2 * p : 2 * p + 1]
        for t in tops[1:]:
            top = jnp.maximum(top, t[2 * p : 2 * p + 1])
        factors = [jnp.exp(t[2 * p : 2 * p + 1] - top) for t in tops]
        total = factors[0] * tops[0][2 * p + 1 : 2 * p + 2]
        for f, t in zip(factors[1:], tops[1:]):
            total = total + f * t[2 * p + 1 : 2 * p + 2]
        merged[2 * p : 2 * p + 1, :] = top + jnp.log(total)
        value = None
        for f, part in zip(factors, parts):
            weight = jnp.transpose(jnp.broadcast_to(f / total, (LANES, LANES)))
            spread = unstacked(weight)
            term = spread * part[:, p * LANES : (p + 1) * LANES].astype(full)
            value = term if value is None else value + term
        answer[:, p * LANES : (p + 1) * LANES] = value


def fill_bias(scalars, bias, rows):
    base, length, count = scalars[0], scalars[1], scalars[3]
    raw = rows + WIN
    pooled = rows // STRIDE + 2 * pool_half

    def block(first, size, valid):
        key = lax.broadcasted_iota(jnp.int32, (size, rows), 0)
        row = lax.broadcasted_iota(jnp.int32, (size, rows), 1)
        bias[pl.ds(first, size), :] = jnp.where(valid(key, row), 0.0, masked_score)

    def raw_valid(key, row):
        place = base - half + key
        near = (key >= row) & (key < row + WIN)
        return near & (place >= 0) & (place < length)

    def pool_valid(key, row):
        place = STRIDE * (key - pool_half)
        near = (place >= row - PWIN // 2) & (place < row + PWIN // 2)
        return near & (base + place >= 0) & (base + place < length)

    def quest_valid(key, row):
        return key < count

    block(0, raw, raw_valid)
    block(raw, pooled, pool_valid)
    block(raw + pooled, QMAX, quest_valid)


def collect(rows, width, qkv, pooled, everything, of):
    raw = rows + WIN
    count = rows // STRIDE + 2 * pool_half
    first = TAIL + rows - half
    quest = TAIL + 3 * rows
    everything[pl.ds(0, raw), :] = qkv[pl.ds(first, raw), of * width : (of + 1) * width]
    everything[pl.ds(raw, count), :] = pooled[:, (of - 1) * width : of * width]
    everything[pl.ds(raw + count, QMAX), :] = qkv[pl.ds(quest, QMAX), of * width : (of + 1) * width]


def lane_masks(rows):
    lane = lax.broadcasted_iota(jnp.int32, (rows, LANES), 1)
    return lane < DH


def only(block, first, keep):
    return jnp.where(first if keep == 0 else jnp.logical_not(first), block, jnp.zeros_like(block))


def stacked(block):
    first = lane_masks(block.shape[0])
    return jnp.concatenate([only(block, first, 0), only(block, first, 1)], axis=0)


def unstacked(block):
    lane = lax.broadcasted_iota(jnp.int32, (QMAX, LANES), 1)
    return jnp.where(lane < DH, block[:QMAX], block[QMAX:])


def attend_kernel(rows, width, devices, live, scalars, qkv, taps, local, pooled, stats, answer,
                  merged, wide, keys, values, bias, numerator, qstats, numerators, many, send_sem,
                  recv_sem):
    pairs = width // LANES
    own = TAIL + rows
    quest = TAIL + 3 * rows
    count = pooled.shape[0]
    begin = own - PWIN // 2 - taps.shape[0] // 2
    qstats[...] = jnp.zeros_like(qstats)

    def ask(p, carry):
        lanes = pl.ds(pl.multiple_of(p * LANES, LANES), LANES)
        question = stacked(qkv[pl.ds(quest, QMAX), lanes] * scale)
        own_key = qkv[pl.ds(own, rows), pl.ds(pl.multiple_of(width + p * LANES, LANES), LANES)]
        own_value = qkv[pl.ds(own, rows), pl.ds(pl.multiple_of(2 * width + p * LANES, LANES), LANES)]
        score = nt(own_key, question)
        top = jnp.max(score, axis=0, keepdims=True)
        weight = jnp.exp(score - top)
        qstats[pl.ds(2 * p, 1), :] = top
        qstats[pl.ds(2 * p + 1, 1), :] = jnp.sum(weight, axis=0, keepdims=True)
        numerator[:, lanes] = unstacked(jnp.transpose(tn(own_value, weight.astype(low)))).astype(low)
        return carry

    lax.fori_loop(0, pairs, ask, 0)
    pieces = ((numerator, numerators), (qstats, many))
    begin_all(devices, live, pieces, send_sem, recv_sem)

    def pool(p, carry):
        lanes = pl.ds(pl.multiple_of(p * LANES, LANES), LANES)
        wide[...] = qkv[pl.ds(0, quest), pl.ds(pl.multiple_of(width + p * LANES, LANES), LANES)].astype(full)
        total = None
        for tap in range(taps.shape[0]):
            term = taps[tap : tap + 1, lanes] * wide[pl.ds(begin + tap, count, stride=STRIDE), :]
            total = term if total is None else total + term
        pooled[:, lanes] = total.astype(low)
        return carry

    lax.fori_loop(0, 2 * pairs, pool, 0)
    collect(rows, width, qkv, pooled, keys, 1)
    collect(rows, width, qkv, pooled, values, 2)
    fill_bias(scalars, bias, rows)
    stats[...] = jnp.zeros_like(stats)
    first = lane_masks(rows)

    def pair(p, carry):
        lanes = pl.ds(pl.multiple_of(p * LANES, LANES), LANES)
        query = qkv[pl.ds(own, rows), lanes] * scale
        key = keys[:, lanes]
        value_t = jnp.transpose(values[:, lanes])
        parts = []
        for head in range(2):
            score = nt(key, only(query, first, head)) + bias[...]
            top = jnp.max(score, axis=0, keepdims=True)
            weight = jnp.exp(score - top)
            total = jnp.sum(weight, axis=0, keepdims=True)
            stats[pl.ds(2 * p + head, 1), :] = top + jnp.log(total)
            parts.append(mm(value_t[head * DH : (head + 1) * DH], weight.astype(low)) / total)
        local[:, lanes] = jnp.transpose(jnp.concatenate(parts, axis=0))
        return carry

    lax.fori_loop(0, pairs, pair, 0)
    finish_all(devices, live, pieces, send_sem, recv_sem)
    merge_questions(numerator, qstats, numerators, many, answer, merged)


def vmem_call(kernel, ident, copies, out_shapes, scratch, scalars, *inputs):
    vmem = pl.BlockSpec(memory_space=pltpu.VMEM)
    return pl.pallas_call(
        kernel,
        out_shape=[jax.ShapeDtypeStruct(s, t) for s, t in out_shapes],
        in_specs=[pl.BlockSpec(memory_space=pltpu.SMEM)] + [vmem] * len(inputs),
        out_specs=[vmem] * len(out_shapes),
        scratch_shapes=[pltpu.VMEM(s, t) for s, t in scratch]
        + [pltpu.SemaphoreType.DMA((copies,))] * 2,
        compiler_params=pltpu.CompilerParams(
            collective_id=ident, has_side_effects=True, vmem_limit_bytes=60 << 20
        ),
    )(scalars, *inputs)


def attend(ident, live, scalars, qkv, taps, rows):
    width = qkv.shape[1] // 3
    devices = lax.axis_size(SEQ)
    heads = width // DH
    pooled = rows // STRIDE + 2 * pool_half
    keys = rows + WIN + pooled + QMAX
    tall = -(-heads // 8) * 8
    return vmem_call(
        functools.partial(attend_kernel, rows, width, devices, live),
        ident,
        2 * (devices - 1),
        (
            ((rows, width), full),
            ((pooled, 2 * width), low),
            ((tall, rows), full),
            ((QMAX, width), full),
            ((tall, LANES), full),
        ),
        (
            ((TAIL + 3 * rows, LANES), full),
            ((keys, width), low),
            ((keys, width), low),
            ((keys, rows), full),
            ((QMAX, width), low),
            ((tall, LANES), full),
            ((devices - 1, QMAX, width), low),
            ((devices - 1, tall, LANES), full),
        ),
        scalars,
        qkv,
        taps,
    )


def attend_back_kernel(rows, width, devices, live, scalars, qkv, taps, pooled, stats, qstats, answer,
                       grad_mixed, grad_part, grads, grad_taps, wide, gwide, keys, values, gkeys,
                       gvalues, bias, grad_answer, grad_parts, send_sem, recv_sem):
    pieces = ((grad_part, grad_parts),)
    begin_all(devices, live, pieces, send_sem, recv_sem)
    pairs = width // LANES
    own = TAIL + rows
    quest = TAIL + 3 * rows
    raw = rows + WIN
    count = pooled.shape[0]
    begin = own - PWIN // 2 - taps.shape[0] // 2
    collect(rows, width, qkv, pooled, keys, 1)
    collect(rows, width, qkv, pooled, values, 2)
    fill_bias(scalars, bias, rows)
    first = lane_masks(rows)
    base, length, start, limit = scalars[0], scalars[1], scalars[2], scalars[3]
    place = base + lax.broadcasted_iota(jnp.int32, (rows, LANES), 0)
    plain = (place < start) | (place >= start + limit)
    grads[:, 0:width] = jnp.zeros((grads.shape[0], width), low)

    def pair(p, carry):
        lanes = pl.ds(pl.multiple_of(p * LANES, LANES), LANES)
        query = qkv[pl.ds(own, rows), lanes] * scale
        grad = jnp.where(plain, grad_mixed[:, lanes], jnp.zeros((rows, LANES), low))
        key = keys[:, lanes]
        value = values[:, lanes]
        key_t = jnp.transpose(key)
        parts = []
        gkey = None
        gvalue = None
        for head in range(2):
            one = only(query, first, head)
            out = only(grad, first, head)
            score = nt(key, one) + bias[...]
            soft = jnp.exp(score - stats[pl.ds(2 * p + head, 1), :])
            grad_soft = nt(value, out)
            delta = jnp.sum(soft * grad_soft, axis=0, keepdims=True)
            grad_score = (soft * (grad_soft - delta)).astype(low)
            more_v = mm(soft.astype(low), out)
            more_k = mm(grad_score, one)
            gvalue = more_v if gvalue is None else gvalue + more_v
            gkey = more_k if gkey is None else gkey + more_k
            parts.append(mm(key_t[head * DH : (head + 1) * DH], grad_score))
        grads[pl.ds(own, rows), lanes] = (
            jnp.transpose(jnp.concatenate(parts, axis=0)) * scale
        ).astype(low)
        gkeys[:, lanes] = gkey
        gvalues[:, lanes] = gvalue
        return carry

    lax.fori_loop(0, pairs, pair, 0)
    finish_all(devices, live, pieces, send_sem, recv_sem)
    grad_answer[...] = slot_sum(grad_part[...], grad_parts).astype(low)

    def ask(p, carry):
        lanes = pl.ds(pl.multiple_of(p * LANES, LANES), LANES)
        question = stacked(qkv[pl.ds(quest, QMAX), lanes] * scale)
        grad_q = grad_answer[:, lanes]
        out = stacked(grad_q)
        own_key = keys[pl.ds(half, rows), lanes]
        own_value = values[pl.ds(half, rows), lanes]
        score = nt(own_key, question)
        soft = jnp.exp(score - qstats[pl.ds(2 * p, 1), :])
        grad_soft = nt(own_value, out)
        product = stacked(grad_q.astype(full) * answer[:, lanes])
        delta = jnp.sum(jnp.transpose(product), axis=0, keepdims=True)
        grad_score = (soft * (grad_soft - delta)).astype(low)
        grads[pl.ds(quest, QMAX), lanes] = (
            unstacked(jnp.transpose(tn(own_key, grad_score))) * scale
        ).astype(low)
        gkeys[pl.ds(half, rows), lanes] += mm(grad_score, question)
        gvalues[pl.ds(half, rows), lanes] += mm(soft.astype(low), out)
        return carry

    lax.fori_loop(0, pairs, ask, 0)
    spot = base - own + lax.broadcasted_iota(jnp.int32, (quest, LANES), 0)
    inside = (spot >= 0) & (spot < length)
    tail = quest - (own - half) - raw

    def unpool(part, at, p):
        lanes = pl.ds(pl.multiple_of(p * LANES, LANES), LANES)
        tapped = pl.ds(pl.multiple_of(at - width + p * LANES, LANES), LANES)
        target = pl.ds(pl.multiple_of(at + p * LANES, LANES), LANES)
        wide[...] = qkv[pl.ds(0, quest), target].astype(full)
        gwide[pl.ds(0, own - half), :] = jnp.zeros((own - half, LANES), full)
        gwide[pl.ds(own - half, raw), :] = part[pl.ds(0, raw), lanes]
        gwide[pl.ds(quest - tail, tail), :] = jnp.zeros((tail, LANES), full)
        gpool = part[pl.ds(raw, count), lanes]
        for tap in range(taps.shape[0]):
            near = pl.ds(begin + tap, count, stride=STRIDE)
            gwide[near, :] += taps[tap : tap + 1, tapped] * gpool
            grad_taps[tap : tap + 1, tapped] = jnp.sum(gpool * wide[near, :], axis=0, keepdims=True)
        grads[pl.ds(0, quest), target] = jnp.where(inside, gwide[...], 0.0).astype(low)
        grads[pl.ds(quest, QMAX), target] = part[pl.ds(raw + count, QMAX), lanes].astype(low)

    def both(p, carry):
        unpool(gkeys, width, p)
        unpool(gvalues, 2 * width, p)
        return carry

    lax.fori_loop(0, pairs, both, 0)


def attend_back(ident, live, scalars, qkv, taps, pooled, stats, qstats, answer, grad_mixed,
                grad_part, rows):
    width = qkv.shape[1] // 3
    devices = lax.axis_size(SEQ)
    count = rows // STRIDE + 2 * pool_half
    keys = rows + WIN + count + QMAX
    span = TAIL + 3 * rows
    return vmem_call(
        functools.partial(attend_back_kernel, rows, width, devices, live),
        ident,
        devices - 1,
        ((qkv.shape, low), (taps.shape, full)),
        (
            ((span, LANES), full),
            ((span, LANES), full),
            ((keys, width), low),
            ((keys, width), low),
            ((keys, width), full),
            ((keys, width), full),
            ((keys, rows), full),
            ((QMAX, width), low),
            ((devices - 1, QMAX, width), low),
        ),
        scalars,
        qkv,
        taps,
        pooled,
        stats,
        qstats,
        answer,
        grad_mixed,
        grad_part,
    )


def reduce_kernel(count, blocks, side, across, n_in, live, *refs):
    ins, refs = refs[:n_in], refs[n_in:]
    tap_grads, vectors, refs = refs[0], refs[1:5], refs[5:]
    outs, little_out, refs = refs[:n_in], refs[n_in], refs[n_in + 1 :]
    first_in, second_in, across_in, little_in, little_slots, little_x, little_y = refs[:7]
    held, made = refs[7:9]
    one, two, over, back, back_two, back_one, tiny, load, store_sem = refs[9:]
    total = len(blocks)
    big, small = side // 2, side // 4
    piece = max(TAIL, small // count)
    owners = small // piece
    me = lax.axis_index(SEQ)
    place = lax.axis_index(DP)
    bit_x, bit_y = lax.rem(place, 2), place // 2
    to_x, to_y = place + 1 - 2 * bit_x, place + 2 - 4 * bit_y

    def ways(b):
        if b % 2 == 0:
            return bit_x, bit_y, to_x, to_y
        return bit_y, bit_x, to_y, to_x

    def view(group, b, row, rows):
        ref, top, left = blocks[b]
        row = pl.multiple_of(top + row, TAIL)
        return group[ref].at[pl.ds(row, rows), left : left + across]

    def final(b, row, rows):
        return made.at[b, pl.ds(pl.multiple_of(row, TAIL), rows)]

    def fetch(b):
        f, s, near, far = ways(b)
        return pltpu.make_async_copy(view(ins, b, f * big, big), held.at[b], load.at[b])

    def keep(b):
        return pltpu.make_async_copy(made.at[b], view(outs, b, 0, side), store_sem.at[b])

    def remote(src, dst, sems, index, axis, peer):
        return pltpu.make_async_remote_copy(
            src_ref=src,
            dst_ref=dst,
            send_sem=sems.at[(0,) + index],
            recv_sem=sems.at[(1,) + index],
            device_id={axis: peer},
            device_id_type=MESH,
        )

    def stage_one(b):
        f, s, near, far = ways(b)
        return remote(view(ins, b, (1 - f) * big, big), first_in.at[b], one, (b,), DP, near)

    def stage_two(b):
        f, s, near, far = ways(b)
        row = pl.multiple_of((1 - s) * small, TAIL)
        return remote(first_in.at[b, pl.ds(row, small)], second_in.at[b], two, (b,), DP, far)

    def spread(b, step):
        peer = lax.rem(me + step, count)
        row = pl.multiple_of(jnp.minimum(peer, owners - 1) * piece, TAIL)
        copy = remote(
            second_in.at[b, pl.ds(row, piece)], across_in.at[b, step - 1], over, (b, step - 1), SEQ, peer
        )
        return copy, peer < owners, me < owners

    def mine(b):
        f, s, near, far = ways(b)
        return f * big + s * small

    def gather(b, step):
        peer = lax.rem(me + step, count)
        row = mine(b) + jnp.minimum(me, owners - 1) * piece
        here = final(b, row, piece)
        copy = remote(here, here, back, (b, step - 1), SEQ, peer)
        return copy, me < owners, lax.rem(me + count - step, count) < owners

    def gather_two(b):
        f, s, near, far = ways(b)
        here = final(b, mine(b), small)
        return remote(here, here, back_two, (b,), DP, far)

    def gather_one(b):
        f, s, near, far = ways(b)
        here = final(b, f * big, big)
        return remote(here, here, back_one, (b,), DP, near)

    def guarded(condition, action):
        if owners == count:
            action()
        else:
            pl.when(condition)(action)

    def begin_one(b):
        stage_one(b).start()
        fetch(b).start()

    def finish_one(b):
        f, s, near, far = ways(b)
        fetch(b).wait()
        stage_one(b).wait_recv()
        own = held[b].astype(full)
        first_in[b] = (first_in[b].astype(full) + own).astype(low)
        stage_two(b).start()

    def finish_two(b):
        f, s, near, far = ways(b)
        stage_two(b).wait_recv()
        own = first_in[b, pl.ds(pl.multiple_of(s * small, TAIL), small)].astype(full)
        second_in[b] = (second_in[b].astype(full) + own).astype(low)
        for step in range(1, count):
            copy, send, take = spread(b, step)
            guarded(send, copy.start)

    def finish_over(b):
        for step in range(1, count):
            copy, send, take = spread(b, step)
            guarded(take, copy.wait_recv)

        def store():
            row = pl.multiple_of(jnp.minimum(me, owners - 1) * piece, TAIL)
            answer = second_in[b, pl.ds(row, piece)].astype(full)
            for step in range(1, count):
                answer = answer + across_in[b, step - 1].astype(full)
            final(b, mine(b) + row, piece)[...] = answer.astype(low)

        guarded(me < owners, store)
        for step in range(1, count):
            copy, send, take = gather(b, step)
            guarded(send, copy.start)

    def finish_back(b):
        for step in range(1, count):
            copy, send, take = gather(b, step)
            guarded(take, copy.wait_recv)
        gather_two(b).start()

    def finish_back_two(b):
        gather_two(b).wait_recv()
        gather_one(b).start()

    def finish_back_one(b):
        gather_one(b).wait_recv()
        keep(b).start()

    def little_copy(step):
        peer = lax.rem(me + step, count)
        return remote(little_in, little_slots.at[step - 1], tiny, (step - 1,), SEQ, peer)

    def little_pair(slot, src, dst, peer):
        return remote(src, dst, tiny, (count - 1 + slot,), DP, peer)

    @pl.when(lax.axis_index(SECTION) == live)
    def _():
        barrier = pltpu.get_barrier_semaphore()
        for step in range(1, count):
            peer = lax.rem(me + step, count)
            pl.semaphore_signal(barrier, inc=1, device_id={SEQ: peer}, device_id_type=MESH)
        for peer in (to_x, to_y):
            pl.semaphore_signal(barrier, inc=1, device_id={DP: peer}, device_id_type=MESH)
        pl.semaphore_wait(barrier, count + 1)

        taps = tap_grads.shape[0]
        little_in[...] = jnp.zeros_like(little_in)
        little_in[0:taps, :] = tap_grads[:, :side]
        little_in[taps : 2 * taps, :] = tap_grads[:, side:]
        for k, vector in enumerate(vectors):
            little_in[2 * taps + k : 2 * taps + k + 1, :] = vector[...]
        for step in range(1, count):
            little_copy(step).start()
        pairs = total // 2
        ahead = 3
        stages = (finish_one, finish_two, finish_over, finish_back, finish_back_two, finish_back_one)
        for k in range(min(ahead, pairs)):
            begin_one(2 * k)
            begin_one(2 * k + 1)
        for turn in range(pairs + len(stages) - 1):
            for depth, stage in enumerate(stages):
                k = turn - depth
                if 0 <= k < pairs:
                    stage(2 * k)
                    stage(2 * k + 1)
                if depth == 0 and turn + ahead < pairs:
                    begin_one(2 * (turn + ahead))
                    begin_one(2 * (turn + ahead) + 1)
            if turn == 0:
                for step in range(1, count):
                    little_copy(step).wait()
                value = little_in[...]
                for step in range(1, count):
                    value = value + little_slots[step - 1]
                little_x[0] = value
                little_pair(0, little_x.at[0], little_x.at[1], to_x).start()
            if turn == 1:
                little_pair(0, little_x.at[0], little_x.at[1], to_x).wait()
                little_y[0] = little_x[0] + little_x[1]
                little_pair(1, little_y.at[0], little_y.at[1], to_y).start()
            if turn == 2:
                little_pair(1, little_y.at[0], little_y.at[1], to_y).wait()
                little_out[...] = little_y[0] + little_y[1]
        for b in range(total):
            stage_one(b).wait_send()
            stage_two(b).wait_send()
            for step in range(1, count):
                copy, send, take = spread(b, step)
                guarded(send, copy.wait_send)
                copy, send, take = gather(b, step)
                guarded(send, copy.wait_send)
            gather_two(b).wait_send()
            gather_one(b).wait_send()
            keep(b).wait()


def unwritten(shapes):
    return pl.pallas_call(
        lambda *refs: None,
        out_shape=[jax.ShapeDtypeStruct(shape, low) for shape in shapes],
        out_specs=[pl.BlockSpec(memory_space=pl.ANY)] * len(shapes),
    )()


def reduce_all(parts, little, ident, live):
    count = lax.axis_size(SEQ)
    tall = -(-(2 * little[0].shape[0] + len(little) - 1) // 8) * 8
    side = min(min(part.shape) for part in parts)
    across = side // 2
    blocks = []
    for k, part in enumerate(parts):
        for top in range(0, part.shape[0], side):
            for left in range(0, part.shape[1], across):
                blocks.append((k, top, left))
    total = len(blocks)
    small = side // 4
    piece = max(TAIL, small // count)
    vmem = pl.BlockSpec(memory_space=pltpu.VMEM)
    sems = pltpu.SemaphoreType.DMA
    return pl.pallas_call(
        functools.partial(reduce_kernel, count, blocks, side, across, len(parts), live),
        out_shape=[jax.ShapeDtypeStruct(part.shape, low) for part in parts]
        + [jax.ShapeDtypeStruct((tall, side), full)],
        in_specs=[pl.BlockSpec(memory_space=pl.ANY)] * len(parts) + [vmem] * len(little),
        out_specs=[pl.BlockSpec(memory_space=pl.ANY)] * len(parts) + [vmem],
        scratch_shapes=[
            pltpu.VMEM((total, side // 2, across), low),
            pltpu.VMEM((total, small, across), low),
            pltpu.VMEM((total, count - 1, piece, across), low),
            pltpu.VMEM((tall, side), full),
            pltpu.VMEM((count - 1, tall, side), full),
            pltpu.VMEM((2, tall, side), full),
            pltpu.VMEM((2, tall, side), full),
            pltpu.VMEM((total, side // 2, across), low),
            pltpu.VMEM((total, side, across), low),
            sems((2, total)),
            sems((2, total)),
            sems((2, total, count - 1)),
            sems((2, total, count - 1)),
            sems((2, total)),
            sems((2, total)),
            sems((2, count + 1)),
            sems((total,)),
            sems((total,)),
        ],
        compiler_params=pltpu.CompilerParams(
            collective_id=ident, has_side_effects=True, vmem_limit_bytes=62 << 20
        ),
    )(*parts, *little)


def layer_forward(tick, live, state_low, params, positions, count):
    qkv_w, output_w, up_w, down_w, taps, gain_one, bias_one, gain_two, bias_two = params
    rows, width = state_low.shape
    base = lax.axis_index(SEQ) * rows
    length = lax.axis_size(SEQ) * rows
    valid = jnp.arange(QMAX, dtype=jnp.int32) < count
    row_pos = base + jnp.arange(rows, dtype=jnp.int32)
    select = (positions[:, None] == row_pos[None, :]) & valid[:, None]
    select_low = select.astype(low)
    scalars = jnp.stack([base, jnp.int32(length), positions[0], count])
    pick = mm(select_low, state_low).astype(low)
    extended = gather_rows(4 * tick, live, state_low, pick)
    normed = norm_rows(extended.astype(full), gain_one, bias_one).astype(low)
    spot = base - TAIL - rows + jnp.arange(extended.shape[0], dtype=jnp.int32)
    inside = ((spot >= 0) & (spot < length)) | (jnp.arange(extended.shape[0]) >= TAIL + 3 * rows)
    qkv = jnp.where(inside[:, None], mm(normed, qkv_w), 0.0).astype(low)
    local, pooled, stats, answer, qstats = attend(4 * tick + 1, live, scalars, qkv, taps, rows)
    is_question = jnp.any(select, axis=0)
    replaced = tn(select_low, answer.astype(low))
    mixed = jnp.where(is_question[:, None], replaced, local).astype(low)
    state = state_low.astype(full)
    middle = state + mm(mixed, output_w)
    normed_two = norm_rows(middle, gain_two, bias_two).astype(low)
    hidden = mm(normed_two, up_w)
    active, slope = gelu_parts(hidden)
    result = middle + mm(active, down_w)
    tape = (state_low, select_low, scalars, normed, qkv, pooled, stats, qstats, answer, mixed,
            middle, normed_two, slope, active)
    return result.astype(low), tape


def layer_backward(tick, live, grad_low, params, tape):
    qkv_w, output_w, up_w, down_w, taps, gain_one, bias_one, gain_two, bias_two = params
    (state_low, select_low, scalars, normed, qkv, pooled, stats, qstats, answer, mixed,
     middle, normed_two, slope, active) = tape
    rows, width = state_low.shape
    grad_out = grad_low.astype(full)
    grad_active = nt(grad_low, down_w)
    grad_hidden = (grad_active * slope.astype(full)).astype(low)
    grad_normed_two = nt(grad_hidden, up_w)
    _, norm_back_two = jax.vjp(norm_rows, middle, gain_two, bias_two)
    grad_middle, g_gain_two, g_bias_two = norm_back_two(grad_normed_two)
    grad_middle = grad_middle + grad_out
    branch = grad_middle.astype(low)
    grad_mixed = nt(branch, output_w).astype(low)
    grad_part = mm(select_low, grad_mixed).astype(low)
    grads, grad_taps = attend_back(
        4 * tick + 2, live, scalars, qkv, taps, pooled, stats, qstats, answer, grad_mixed,
        grad_part, rows
    )
    grad_extended = nt(grads, qkv_w).astype(low)
    grad_normed, grad_picked = return_rows(4 * tick + 3, live, grad_extended, rows)
    grad_normed = grad_normed + tn(select_low, grad_picked.astype(low))
    _, norm_back_one = jax.vjp(norm_rows, state_low.astype(full), gain_one, bias_one)
    grad_state, g_gain_one, g_bias_one = norm_back_one(grad_normed)
    small = (grad_taps, g_gain_one, g_bias_one, g_gain_two, g_bias_two)
    big = ((normed, grads), (mixed, branch), (normed_two, grad_hidden), (active, grad_low))
    return (grad_state + grad_middle).astype(low), big, small


def to_partner(block):
    return lax.ppermute(block, SECTION, [(0, 1), (1, 0)])


def per_device(
    inputs,
    cotangent,
    question_positions,
    question_counts,
    query_weight,
    key_weight,
    value_weight,
    output_weight,
    up_weight,
    down_weight,
    key_pool,
    value_pool,
    attn_norm_gain,
    attn_norm_bias,
    ffn_norm_gain,
    ffn_norm_bias,
):
    params = (
        jnp.concatenate([query_weight[0], key_weight[0], value_weight[0]], axis=1),
        output_weight[0],
        up_weight[0],
        down_weight[0],
        jnp.concatenate([key_pool[0], value_pool[0]], axis=1),
        attn_norm_gain[0],
        attn_norm_bias[0],
        ffn_norm_gain[0],
        ffn_norm_bias[0],
    )
    section = lax.axis_index(SECTION)
    micro, rows, width = inputs.shape

    def alive(tick):
        if tick == 0:
            return 0
        return 1 if tick == micro else None

    received = jnp.zeros((rows, width), low)
    tapes = []
    made = []
    for tick in range(micro + 1):
        slot = jnp.clip(tick - section, 0, micro - 1)
        layer_in = jnp.where(section == 0, inputs[min(tick, micro - 1)], received)
        result, tape = layer_forward(
            tick, alive(tick), layer_in, params, question_positions[slot], question_counts[slot]
        )
        tapes.append(tape)
        made.append(result)
        if tick < micro:
            received = to_partner(result)
    produced = jnp.where(section == 0, jnp.stack(made[:micro]), jnp.stack(made[1:]))
    grad_in = jnp.zeros((rows, width), low)
    back = []
    bigs = []
    smalls = []
    reduced = []

    def reduce_section(which):
        ticks = range(1 - which, micro + 1 - which)

        def sums():
            parts = []
            for k in range(len(bigs[0])):
                left = jnp.concatenate([bigs[t][k][0] for t in ticks], axis=0)
                right = jnp.concatenate([bigs[t][k][1] for t in ticks], axis=0)
                parts.append(tn(left, right).astype(low))
            return parts

        def nothing():
            return list(unwritten([(a.shape[1], b.shape[1]) for a, b in bigs[micro - 1]]))

        parts = lax.cond(section == which, sums, nothing)
        little = []
        for k in range(len(smalls[0])):
            total = smalls[ticks[0]][k]
            for t in ticks[1:]:
                total = total + smalls[t][k]
            little.append(total.reshape(-1, total.shape[-1]))
        reduced.append(reduce_all(parts, little, 4 * micro + 4 + which, which))

    for tick in range(micro + 1):
        mirror = micro - tick
        grad_out = jnp.where(section == 1, cotangent[max(mirror - 1, 0)], grad_in)
        grad_state, big, small = layer_backward(
            mirror, alive(mirror), grad_out, params, tapes[mirror]
        )
        back.append(grad_state)
        bigs.append(big)
        smalls.append(small)
        if tick < micro:
            grad_in = to_partner(grad_state)
        if tick == micro - 1:
            grad_in, bigs, smalls = lax.optimization_barrier((grad_in, bigs, smalls))
            reduce_section(1)
            grad_in, reduced[0] = lax.optimization_barrier((grad_in, reduced[0]))
    back_grads = jnp.where(
        section == 0, jnp.stack(back[1:][::-1]), jnp.stack(back[:micro][::-1])
    )
    reduce_section(0)
    *sums, little = [
        jnp.where(section == 0, mine, other).astype(full) for other, mine in zip(*reduced)
    ]
    taps = key_pool.shape[1]
    return (
        produced[None],
        back_grads[None],
        sums[0][None, :, :width],
        sums[0][None, :, width : 2 * width],
        sums[0][None, :, 2 * width :],
        sums[1][None],
        sums[2][None],
        sums[3][None],
        little[None, :taps],
        little[None, taps : 2 * taps],
        little[2 * taps : 2 * taps + 1],
        little[2 * taps + 1 : 2 * taps + 2],
        little[2 * taps + 2 : 2 * taps + 3],
        little[2 * taps + 3 : 2 * taps + 4],
    )


def solution(mesh):
    rows = P(DP, SEQ, None)
    matrix = P(SECTION, None, None)
    vector = P(SECTION, None)
    result = P(SECTION, DP, SEQ, None)
    return jax.shard_map(
        per_device,
        mesh=mesh,
        in_specs=(rows, rows, P(DP, None), P(DP)) + (matrix,) * 8 + (vector,) * 4,
        out_specs=(result, result) + (matrix,) * 8 + (vector,) * 4,
        check_vma=False,
    )
```

```python
import functools
import math

import jax
import jax.numpy as jnp
from jax import lax
from jax.experimental import pallas as pl
from jax.experimental.pallas import tpu as pltpu
from jax.sharding import PartitionSpec as P

DH = 64
WIN = 128
PWIN = 512
STRIDE = 4
QMAX = 64
TAIL = 16
LANES = 128

epsilon = 1e-05
masked_score = -1e30
scale = 1.0 / math.sqrt(DH)
half = WIN // 2
pool_half = PWIN // (2 * STRIDE)
low = jnp.bfloat16
full = jnp.float32
SECTION, DP, SEQ = "section", "dp", "seq"
MESH = pl.DeviceIdType.MESH


def norm_rows(state, gain, shift):
    average = jnp.mean(state, axis=-1, keepdims=True)
    centred = state - average
    variance = jnp.mean(centred * centred, axis=-1, keepdims=True)
    return centred * lax.rsqrt(variance + epsilon) * gain + shift


def gelu_parts(value):
    spread = 0.5 + 0.5 * lax.erf(value * math.sqrt(0.5))
    slope = spread + value * jnp.exp(-0.5 * value * value) * (1.0 / math.sqrt(2.0 * math.pi))
    return (value * spread).astype(low), slope.astype(low)


def mm(left, right):
    return jnp.dot(left, right, preferred_element_type=full)


def tn(left, right):
    return lax.dot_general(left, right, (((0,), (0,)), ((), ())), preferred_element_type=full)


def nt(left, right):
    return lax.dot_general(left, right, (((1,), (1,)), ((), ())), preferred_element_type=full)


def exchange_kernel(count, plan, live, reduce, n_in, n_out, *refs):
    ins, outs = refs[:n_in], refs[n_in : n_in + n_out]
    send_sem, recv_sem, keep_sem = refs[n_in + n_out : n_in + n_out + 3]
    slots = refs[n_in + n_out + 3 :]
    me = lax.axis_index(SEQ)

    def run():
        barrier = pltpu.get_barrier_semaphore()
        for step in range(1, count):
            peer = lax.rem(me + step, count)
            pl.semaphore_signal(barrier, inc=1, device_id={SEQ: peer}, device_id_type=MESH)
        pl.semaphore_wait(barrier, count - 1)
        jobs = []
        sem = 0
        for src, first, rows, shift, dst, at in plan:
            if shift is None:
                buffer = slots[dst]
                for step in range(1, count):
                    peer = lax.rem(me + step, count)
                    copy = pltpu.make_async_remote_copy(
                        src_ref=ins[src].at[pl.ds(first, rows)],
                        dst_ref=buffer.at[step - 1],
                        send_sem=send_sem.at[sem],
                        recv_sem=recv_sem.at[sem],
                        device_id={SEQ: peer},
                        device_id_type=MESH,
                    )
                    copy.start()
                    jobs.append((copy, None, None))
                    sem += 1
            else:
                target, source = me + shift, me - shift
                can_send = (target >= 0) & (target < count)
                can_take = (source >= 0) & (source < count)
                copy = pltpu.make_async_remote_copy(
                    src_ref=ins[src].at[pl.ds(first, rows)],
                    dst_ref=outs[dst].at[pl.ds(at, rows)],
                    send_sem=send_sem.at[sem],
                    recv_sem=recv_sem.at[sem],
                    device_id={SEQ: jnp.clip(target, 0, count - 1)},
                    device_id_type=MESH,
                )

                @pl.when(can_send)
                def _():
                    copy.start()

                @pl.when(jnp.logical_not(can_take))
                def _():
                    outs[dst][pl.ds(at, rows), :] = jnp.zeros((rows, outs[dst].shape[1]), outs[dst].dtype)

                jobs.append((copy, can_send, can_take))
                sem += 1
        for copy, can_send, can_take in jobs:
            if can_send is None:
                copy.wait_send()
                copy.wait_recv()
            else:
                pl.when(can_send)(copy.wait_send)
                pl.when(can_take)(copy.wait_recv)

    if live is None:
        run()
    else:
        on = lax.axis_index(SECTION) == live
        pl.when(on)(run)

        @pl.when(jnp.logical_not(on))
        def _():
            for out in outs:
                out[...] = jnp.zeros(out.shape, out.dtype)
            for buffer in slots:
                buffer[...] = jnp.zeros(buffer.shape, buffer.dtype)

    reduce(ins, outs, slots)


def exchange(ident, live, inputs, plan, out_shapes, slot_shapes, reduce):
    count = lax.axis_size(SEQ)
    copies = sum(count - 1 if item[3] is None else 1 for item in plan)
    vmem = pl.BlockSpec(memory_space=pltpu.VMEM)
    kernel = functools.partial(
        exchange_kernel, count, plan, live, reduce, len(inputs), len(out_shapes)
    )
    return pl.pallas_call(
        kernel,
        out_shape=[jax.ShapeDtypeStruct(s, t) for s, t in out_shapes],
        in_specs=[vmem] * len(inputs),
        out_specs=[vmem] * len(out_shapes),
        scratch_shapes=[
            pltpu.SemaphoreType.DMA((copies,)),
            pltpu.SemaphoreType.DMA((copies,)),
            pltpu.SemaphoreType.DMA((1,)),
        ]
        + [pltpu.VMEM((count - 1,) + s, t) for s, t in slot_shapes],
        compiler_params=pltpu.CompilerParams(collective_id=ident, has_side_effects=True),
    )(*inputs)


def slot_sum(own, slots):
    total = own.astype(full)
    for k in range(slots.shape[0]):
        total = total + slots[k].astype(full)
    return total


def gather_rows(ident, live, state, pick):
    rows, width = state.shape
    own = TAIL + rows
    right = own + rows
    quest = right + rows
    plan = (
        (1, 0, QMAX, None, 0, 0),
        (0, rows - TAIL, TAIL, 2, 0, 0),
        (0, 0, rows, -1, 0, right),
        (0, 0, rows, 1, 0, TAIL),
    )

    def reduce(ins, outs, slots):
        outs[0][pl.ds(own, rows), :] = ins[0][...]
        outs[0][pl.ds(quest, QMAX), :] = slot_sum(ins[1][...], slots[0]).astype(low)

    return exchange(
        ident,
        live,
        (state, pick),
        plan,
        (((quest + QMAX, width), low),),
        (((QMAX, width), low),),
        reduce,
    )[0]


def return_rows(ident, live, grads, rows):
    width = grads.shape[1]
    own = TAIL + rows
    right = own + rows
    quest = right + rows
    plan = (
        (0, quest, QMAX, None, 0, 0),
        (0, 0, TAIL, -2, 4, 0),
        (0, TAIL, rows, -1, 2, 0),
        (0, right, rows, 1, 3, 0),
    )

    def reduce(ins, outs, slots):
        total = ins[0][pl.ds(own, rows), :].astype(full)
        total = total + outs[2][...].astype(full) + outs[3][...].astype(full)
        outs[0][...] = total
        outs[0][pl.ds(rows - TAIL, TAIL), :] += outs[4][...].astype(full)
        outs[1][...] = slot_sum(ins[0][pl.ds(quest, QMAX), :], slots[0])

    return exchange(
        ident,
        live,
        (grads,),
        plan,
        (
            ((rows, width), full),
            ((QMAX, width), full),
            ((rows, width), low),
            ((rows, width), low),
            ((TAIL, width), low),
        ),
        (((QMAX, width), low),),
        reduce,
    )[:2]


def broadcast(count, pieces, send_sem, recv_sem):
    me = lax.axis_index(SEQ)
    copies = []
    for k, (src, slots) in enumerate(pieces):
        for step in range(1, count):
            index = k * (count - 1) + step - 1
            copies.append(
                pltpu.make_async_remote_copy(
                    src_ref=src,
                    dst_ref=slots.at[step - 1],
                    send_sem=send_sem.at[index],
                    recv_sem=recv_sem.at[index],
                    device_id={SEQ: lax.rem(me + step, count)},
                    device_id_type=MESH,
                )
            )
    return copies


def greet(count):
    me = lax.axis_index(SEQ)
    barrier = pltpu.get_barrier_semaphore()
    for step in range(1, count):
        peer = lax.rem(me + step, count)
        pl.semaphore_signal(barrier, inc=1, device_id={SEQ: peer}, device_id_type=MESH)
    pl.semaphore_wait(barrier, count - 1)


def when_live(live, action):
    if live is None:
        action()
    else:
        pl.when(lax.axis_index(SECTION) == live)(action)


def begin_all(count, live, pieces, send_sem, recv_sem):
    def start():
        greet(count)
        for copy in broadcast(count, pieces, send_sem, recv_sem):
            copy.start()

    when_live(live, start)


def finish_all(count, live, pieces, send_sem, recv_sem):
    def finish():
        for copy in broadcast(count, pieces, send_sem, recv_sem):
            copy.wait()

    when_live(live, finish)
    if live is not None:

        @pl.when(lax.axis_index(SECTION) != live)
        def _():
            for _, slots in pieces:
                slots[...] = jnp.zeros(slots.shape, slots.dtype)


def merge_questions(numerator, stats, numerators, many, answer, merged):
    tops = [stats[...]] + [many[k] for k in range(many.shape[0])]
    parts = [numerator] + [numerators.at[k] for k in range(numerators.shape[0])]
    merged[...] = jnp.zeros_like(merged)
    for p in range(numerator.shape[1] // LANES):
        top = tops[0][2 * p : 2 * p + 1]
        for t in tops[1:]:
            top = jnp.maximum(top, t[2 * p : 2 * p + 1])
        factors = [jnp.exp(t[2 * p : 2 * p + 1] - top) for t in tops]
        total = factors[0] * tops[0][2 * p + 1 : 2 * p + 2]
        for f, t in zip(factors[1:], tops[1:]):
            total = total + f * t[2 * p + 1 : 2 * p + 2]
        merged[2 * p : 2 * p + 1, :] = top + jnp.log(total)
        value = None
        for f, part in zip(factors, parts):
            weight = jnp.transpose(jnp.broadcast_to(f / total, (LANES, LANES)))
            spread = unstacked(weight)
            term = spread * part[:, p * LANES : (p + 1) * LANES].astype(full)
            value = term if value is None else value + term
        answer[:, p * LANES : (p + 1) * LANES] = value


def fill_bias(scalars, bias, rows):
    base, length, count = scalars[0], scalars[1], scalars[3]
    raw = rows + WIN
    pooled = rows // STRIDE + 2 * pool_half

    def block(first, size, valid):
        key = lax.broadcasted_iota(jnp.int32, (size, rows), 0)
        row = lax.broadcasted_iota(jnp.int32, (size, rows), 1)
        bias[pl.ds(first, size), :] = jnp.where(valid(key, row), 0.0, masked_score)

    def raw_valid(key, row):
        place = base - half + key
        near = (key >= row) & (key < row + WIN)
        return near & (place >= 0) & (place < length)

    def pool_valid(key, row):
        place = STRIDE * (key - pool_half)
        near = (place >= row - PWIN // 2) & (place < row + PWIN // 2)
        return near & (base + place >= 0) & (base + place < length)

    def quest_valid(key, row):
        return key < count

    block(0, raw, raw_valid)
    block(raw, pooled, pool_valid)
    block(raw + pooled, QMAX, quest_valid)


def collect(rows, width, qkv, pooled, everything, of):
    raw = rows + WIN
    count = rows // STRIDE + 2 * pool_half
    first = TAIL + rows - half
    quest = TAIL + 3 * rows
    everything[pl.ds(0, raw), :] = qkv[pl.ds(first, raw), of * width : (of + 1) * width]
    everything[pl.ds(raw, count), :] = pooled[:, (of - 1) * width : of * width]
    everything[pl.ds(raw + count, QMAX), :] = qkv[pl.ds(quest, QMAX), of * width : (of + 1) * width]


def lane_masks(rows):
    lane = lax.broadcasted_iota(jnp.int32, (rows, LANES), 1)
    return lane < DH


def only(block, first, keep):
    return jnp.where(first if keep == 0 else jnp.logical_not(first), block, jnp.zeros_like(block))


def stacked(block):
    first = lane_masks(block.shape[0])
    return jnp.concatenate([only(block, first, 0), only(block, first, 1)], axis=0)


def unstacked(block):
    lane = lax.broadcasted_iota(jnp.int32, (QMAX, LANES), 1)
    return jnp.where(lane < DH, block[:QMAX], block[QMAX:])


def attend_kernel(rows, width, devices, live, scalars, qkv, taps, local, pooled, stats, answer,
                  merged, wide, keys, values, bias, numerator, qstats, numerators, many, send_sem,
                  recv_sem):
    pairs = width // LANES
    own = TAIL + rows
    quest = TAIL + 3 * rows
    count = pooled.shape[0]
    begin = own - PWIN // 2 - taps.shape[0] // 2
    qstats[...] = jnp.zeros_like(qstats)

    def ask(p, carry):
        lanes = pl.ds(pl.multiple_of(p * LANES, LANES), LANES)
        question = stacked(qkv[pl.ds(quest, QMAX), lanes] * scale)
        own_key = qkv[pl.ds(own, rows), pl.ds(pl.multiple_of(width + p * LANES, LANES), LANES)]
        own_value = qkv[pl.ds(own, rows), pl.ds(pl.multiple_of(2 * width + p * LANES, LANES), LANES)]
        score = nt(own_key, question)
        top = jnp.max(score, axis=0, keepdims=True)
        weight = jnp.exp(score - top)
        qstats[pl.ds(2 * p, 1), :] = top
        qstats[pl.ds(2 * p + 1, 1), :] = jnp.sum(weight, axis=0, keepdims=True)
        numerator[:, lanes] = unstacked(jnp.transpose(tn(own_value, weight.astype(low)))).astype(low)
        return carry

    lax.fori_loop(0, pairs, ask, 0)
    pieces = ((numerator, numerators), (qstats, many))
    begin_all(devices, live, pieces, send_sem, recv_sem)

    def pool(p, carry):
        lanes = pl.ds(pl.multiple_of(p * LANES, LANES), LANES)
        wide[...] = qkv[pl.ds(0, quest), pl.ds(pl.multiple_of(width + p * LANES, LANES), LANES)].astype(full)
        total = None
        for tap in range(taps.shape[0]):
            term = taps[tap : tap + 1, lanes] * wide[pl.ds(begin + tap, count, stride=STRIDE), :]
            total = term if total is None else total + term
        pooled[:, lanes] = total.astype(low)
        return carry

    lax.fori_loop(0, 2 * pairs, pool, 0)
    collect(rows, width, qkv, pooled, keys, 1)
    collect(rows, width, qkv, pooled, values, 2)
    fill_bias(scalars, bias, rows)
    stats[...] = jnp.zeros_like(stats)
    first = lane_masks(rows)

    def pair(p, carry):
        lanes = pl.ds(pl.multiple_of(p * LANES, LANES), LANES)
        query = qkv[pl.ds(own, rows), lanes] * scale
        key = keys[:, lanes]
        value_t = jnp.transpose(values[:, lanes])
        parts = []
        for head in range(2):
            score = nt(key, only(query, first, head)) + bias[...]
            top = jnp.max(score, axis=0, keepdims=True)
            weight = jnp.exp(score - top)
            total = jnp.sum(weight, axis=0, keepdims=True)
            stats[pl.ds(2 * p + head, 1), :] = top + jnp.log(total)
            parts.append(mm(value_t[head * DH : (head + 1) * DH], weight.astype(low)) / total)
        local[:, lanes] = jnp.transpose(jnp.concatenate(parts, axis=0))
        return carry

    lax.fori_loop(0, pairs, pair, 0)
    finish_all(devices, live, pieces, send_sem, recv_sem)
    merge_questions(numerator, qstats, numerators, many, answer, merged)


def vmem_call(kernel, ident, copies, out_shapes, scratch, scalars, *inputs):
    vmem = pl.BlockSpec(memory_space=pltpu.VMEM)
    return pl.pallas_call(
        kernel,
        out_shape=[jax.ShapeDtypeStruct(s, t) for s, t in out_shapes],
        in_specs=[pl.BlockSpec(memory_space=pltpu.SMEM)] + [vmem] * len(inputs),
        out_specs=[vmem] * len(out_shapes),
        scratch_shapes=[pltpu.VMEM(s, t) for s, t in scratch]
        + [pltpu.SemaphoreType.DMA((copies,))] * 2,
        compiler_params=pltpu.CompilerParams(
            collective_id=ident, has_side_effects=True, vmem_limit_bytes=60 << 20
        ),
    )(scalars, *inputs)


def attend(ident, live, scalars, qkv, taps, rows):
    width = qkv.shape[1] // 3
    devices = lax.axis_size(SEQ)
    heads = width // DH
    pooled = rows // STRIDE + 2 * pool_half
    keys = rows + WIN + pooled + QMAX
    tall = -(-heads // 8) * 8
    return vmem_call(
        functools.partial(attend_kernel, rows, width, devices, live),
        ident,
        2 * (devices - 1),
        (
            ((rows, width), full),
            ((pooled, 2 * width), low),
            ((tall, rows), full),
            ((QMAX, width), full),
            ((tall, LANES), full),
        ),
        (
            ((TAIL + 3 * rows, LANES), full),
            ((keys, width), low),
            ((keys, width), low),
            ((keys, rows), full),
            ((QMAX, width), low),
            ((tall, LANES), full),
            ((devices - 1, QMAX, width), low),
            ((devices - 1, tall, LANES), full),
        ),
        scalars,
        qkv,
        taps,
    )


def attend_back_kernel(rows, width, devices, live, scalars, qkv, taps, pooled, stats, qstats, answer,
                       grad_mixed, grad_part, grads, grad_taps, wide, gwide, keys, values, gkeys,
                       gvalues, bias, grad_answer, grad_parts, send_sem, recv_sem):
    pieces = ((grad_part, grad_parts),)
    begin_all(devices, live, pieces, send_sem, recv_sem)
    pairs = width // LANES
    own = TAIL + rows
    quest = TAIL + 3 * rows
    raw = rows + WIN
    count = pooled.shape[0]
    begin = own - PWIN // 2 - taps.shape[0] // 2
    collect(rows, width, qkv, pooled, keys, 1)
    collect(rows, width, qkv, pooled, values, 2)
    fill_bias(scalars, bias, rows)
    first = lane_masks(rows)
    base, length, start, limit = scalars[0], scalars[1], scalars[2], scalars[3]
    place = base + lax.broadcasted_iota(jnp.int32, (rows, LANES), 0)
    plain = (place < start) | (place >= start + limit)
    grads[:, 0:width] = jnp.zeros((grads.shape[0], width), low)

    def pair(p, carry):
        lanes = pl.ds(pl.multiple_of(p * LANES, LANES), LANES)
        query = qkv[pl.ds(own, rows), lanes] * scale
        grad = jnp.where(plain, grad_mixed[:, lanes], jnp.zeros((rows, LANES), low))
        key = keys[:, lanes]
        value = values[:, lanes]
        key_t = jnp.transpose(key)
        parts = []
        gkey = None
        gvalue = None
        for head in range(2):
            one = only(query, first, head)
            out = only(grad, first, head)
            score = nt(key, one) + bias[...]
            soft = jnp.exp(score - stats[pl.ds(2 * p + head, 1), :])
            grad_soft = nt(value, out)
            delta = jnp.sum(soft * grad_soft, axis=0, keepdims=True)
            grad_score = (soft * (grad_soft - delta)).astype(low)
            more_v = mm(soft.astype(low), out)
            more_k = mm(grad_score, one)
            gvalue = more_v if gvalue is None else gvalue + more_v
            gkey = more_k if gkey is None else gkey + more_k
            parts.append(mm(key_t[head * DH : (head + 1) * DH], grad_score))
        grads[pl.ds(own, rows), lanes] = (
            jnp.transpose(jnp.concatenate(parts, axis=0)) * scale
        ).astype(low)
        gkeys[:, lanes] = gkey
        gvalues[:, lanes] = gvalue
        return carry

    lax.fori_loop(0, pairs, pair, 0)
    finish_all(devices, live, pieces, send_sem, recv_sem)
    grad_answer[...] = slot_sum(grad_part[...], grad_parts).astype(low)

    def ask(p, carry):
        lanes = pl.ds(pl.multiple_of(p * LANES, LANES), LANES)
        question = stacked(qkv[pl.ds(quest, QMAX), lanes] * scale)
        grad_q = grad_answer[:, lanes]
        out = stacked(grad_q)
        own_key = keys[pl.ds(half, rows), lanes]
        own_value = values[pl.ds(half, rows), lanes]
        score = nt(own_key, question)
        soft = jnp.exp(score - qstats[pl.ds(2 * p, 1), :])
        grad_soft = nt(own_value, out)
        product = stacked(grad_q.astype(full) * answer[:, lanes])
        delta = jnp.sum(jnp.transpose(product), axis=0, keepdims=True)
        grad_score = (soft * (grad_soft - delta)).astype(low)
        grads[pl.ds(quest, QMAX), lanes] = (
            unstacked(jnp.transpose(tn(own_key, grad_score))) * scale
        ).astype(low)
        gkeys[pl.ds(half, rows), lanes] += mm(grad_score, question)
        gvalues[pl.ds(half, rows), lanes] += mm(soft.astype(low), out)
        return carry

    lax.fori_loop(0, pairs, ask, 0)
    spot = base - own + lax.broadcasted_iota(jnp.int32, (quest, LANES), 0)
    inside = (spot >= 0) & (spot < length)
    tail = quest - (own - half) - raw

    def unpool(part, at, p):
        lanes = pl.ds(pl.multiple_of(p * LANES, LANES), LANES)
        tapped = pl.ds(pl.multiple_of(at - width + p * LANES, LANES), LANES)
        target = pl.ds(pl.multiple_of(at + p * LANES, LANES), LANES)
        wide[...] = qkv[pl.ds(0, quest), target].astype(full)
        gwide[pl.ds(0, own - half), :] = jnp.zeros((own - half, LANES), full)
        gwide[pl.ds(own - half, raw), :] = part[pl.ds(0, raw), lanes]
        gwide[pl.ds(quest - tail, tail), :] = jnp.zeros((tail, LANES), full)
        gpool = part[pl.ds(raw, count), lanes]
        for tap in range(taps.shape[0]):
            near = pl.ds(begin + tap, count, stride=STRIDE)
            gwide[near, :] += taps[tap : tap + 1, tapped] * gpool
            grad_taps[tap : tap + 1, tapped] = jnp.sum(gpool * wide[near, :], axis=0, keepdims=True)
        grads[pl.ds(0, quest), target] = jnp.where(inside, gwide[...], 0.0).astype(low)
        grads[pl.ds(quest, QMAX), target] = part[pl.ds(raw + count, QMAX), lanes].astype(low)

    def both(p, carry):
        unpool(gkeys, width, p)
        unpool(gvalues, 2 * width, p)
        return carry

    lax.fori_loop(0, pairs, both, 0)


def attend_back(ident, live, scalars, qkv, taps, pooled, stats, qstats, answer, grad_mixed,
                grad_part, rows):
    width = qkv.shape[1] // 3
    devices = lax.axis_size(SEQ)
    count = rows // STRIDE + 2 * pool_half
    keys = rows + WIN + count + QMAX
    span = TAIL + 3 * rows
    return vmem_call(
        functools.partial(attend_back_kernel, rows, width, devices, live),
        ident,
        devices - 1,
        ((qkv.shape, low), (taps.shape, full)),
        (
            ((span, LANES), full),
            ((span, LANES), full),
            ((keys, width), low),
            ((keys, width), low),
            ((keys, width), full),
            ((keys, width), full),
            ((keys, rows), full),
            ((QMAX, width), low),
            ((devices - 1, QMAX, width), low),
        ),
        scalars,
        qkv,
        taps,
        pooled,
        stats,
        qstats,
        answer,
        grad_mixed,
        grad_part,
    )


def reduce_kernel(count, blocks, side, across, n_in, live, *refs):
    ins, refs = refs[:n_in], refs[n_in:]
    tap_grads, vectors, refs = refs[0], refs[1:5], refs[5:]
    outs, little_out, refs = refs[:n_in], refs[n_in], refs[n_in + 1 :]
    first_in, second_in, across_in, little_in, little_slots, little_x, little_y = refs[:7]
    held, made = refs[7:9]
    one, two, over, back, back_two, back_one, tiny, load, store_sem = refs[9:]
    total = len(blocks)
    big, small = side // 2, side // 4
    piece = max(TAIL, small // count)
    owners = small // piece
    me = lax.axis_index(SEQ)
    place = lax.axis_index(DP)
    bit_x, bit_y = lax.rem(place, 2), place // 2
    to_x, to_y = place + 1 - 2 * bit_x, place + 2 - 4 * bit_y

    def ways(b):
        if b % 2 == 0:
            return bit_x, bit_y, to_x, to_y
        return bit_y, bit_x, to_y, to_x

    def view(group, b, row, rows):
        ref, top, left = blocks[b]
        row = pl.multiple_of(top + row, TAIL)
        return group[ref].at[pl.ds(row, rows), left : left + across]

    def final(b, row, rows):
        return made.at[b, pl.ds(pl.multiple_of(row, TAIL), rows)]

    def fetch(b):
        f, s, near, far = ways(b)
        return pltpu.make_async_copy(view(ins, b, f * big, big), held.at[b], load.at[b])

    def keep(b):
        return pltpu.make_async_copy(made.at[b], view(outs, b, 0, side), store_sem.at[b])

    def remote(src, dst, sems, index, axis, peer):
        return pltpu.make_async_remote_copy(
            src_ref=src,
            dst_ref=dst,
            send_sem=sems.at[(0,) + index],
            recv_sem=sems.at[(1,) + index],
            device_id={axis: peer},
            device_id_type=MESH,
        )

    def stage_one(b):
        f, s, near, far = ways(b)
        return remote(view(ins, b, (1 - f) * big, big), first_in.at[b], one, (b,), DP, near)

    def stage_two(b):
        f, s, near, far = ways(b)
        row = pl.multiple_of((1 - s) * small, TAIL)
        return remote(first_in.at[b, pl.ds(row, small)], second_in.at[b], two, (b,), DP, far)

    def spread(b, step):
        peer = lax.rem(me + step, count)
        row = pl.multiple_of(jnp.minimum(peer, owners - 1) * piece, TAIL)
        copy = remote(
            second_in.at[b, pl.ds(row, piece)], across_in.at[b, step - 1], over, (b, step - 1), SEQ, peer
        )
        return copy, peer < owners, me < owners

    def mine(b):
        f, s, near, far = ways(b)
        return f * big + s * small

    def gather(b, step):
        peer = lax.rem(me + step, count)
        row = mine(b) + jnp.minimum(me, owners - 1) * piece
        here = final(b, row, piece)
        copy = remote(here, here, back, (b, step - 1), SEQ, peer)
        return copy, me < owners, lax.rem(me + count - step, count) < owners

    def gather_two(b):
        f, s, near, far = ways(b)
        here = final(b, mine(b), small)
        return remote(here, here, back_two, (b,), DP, far)

    def gather_one(b):
        f, s, near, far = ways(b)
        here = final(b, f * big, big)
        return remote(here, here, back_one, (b,), DP, near)

    def guarded(condition, action):
        if owners == count:
            action()
        else:
            pl.when(condition)(action)

    def begin_one(b):
        stage_one(b).start()
        fetch(b).start()

    def finish_one(b):
        f, s, near, far = ways(b)
        fetch(b).wait()
        stage_one(b).wait_recv()
        own = held[b].astype(full)
        first_in[b] = (first_in[b].astype(full) + own).astype(low)
        stage_two(b).start()

    def finish_two(b):
        f, s, near, far = ways(b)
        stage_two(b).wait_recv()
        own = first_in[b, pl.ds(pl.multiple_of(s * small, TAIL), small)].astype(full)
        second_in[b] = (second_in[b].astype(full) + own).astype(low)
        for step in range(1, count):
            copy, send, take = spread(b, step)
            guarded(send, copy.start)

    def finish_over(b):
        for step in range(1, count):
            copy, send, take = spread(b, step)
            guarded(take, copy.wait_recv)

        def store():
            row = pl.multiple_of(jnp.minimum(me, owners - 1) * piece, TAIL)
            answer = second_in[b, pl.ds(row, piece)].astype(full)
            for step in range(1, count):
                answer = answer + across_in[b, step - 1].astype(full)
            final(b, mine(b) + row, piece)[...] = answer.astype(low)

        guarded(me < owners, store)
        for step in range(1, count):
            copy, send, take = gather(b, step)
            guarded(send, copy.start)

    def finish_back(b):
        for step in range(1, count):
            copy, send, take = gather(b, step)
            guarded(take, copy.wait_recv)
        gather_two(b).start()

    def finish_back_two(b):
        gather_two(b).wait_recv()
        gather_one(b).start()

    def finish_back_one(b):
        gather_one(b).wait_recv()
        keep(b).start()

    def little_copy(step):
        peer = lax.rem(me + step, count)
        return remote(little_in, little_slots.at[step - 1], tiny, (step - 1,), SEQ, peer)

    def little_pair(slot, src, dst, peer):
        return remote(src, dst, tiny, (count - 1 + slot,), DP, peer)

    @pl.when(lax.axis_index(SECTION) == live)
    def _():
        barrier = pltpu.get_barrier_semaphore()
        for step in range(1, count):
            peer = lax.rem(me + step, count)
            pl.semaphore_signal(barrier, inc=1, device_id={SEQ: peer}, device_id_type=MESH)
        for peer in (to_x, to_y):
            pl.semaphore_signal(barrier, inc=1, device_id={DP: peer}, device_id_type=MESH)
        pl.semaphore_wait(barrier, count + 1)

        taps = tap_grads.shape[0]
        little_in[...] = jnp.zeros_like(little_in)
        little_in[0:taps, :] = tap_grads[:, :side]
        little_in[taps : 2 * taps, :] = tap_grads[:, side:]
        for k, vector in enumerate(vectors):
            little_in[2 * taps + k : 2 * taps + k + 1, :] = vector[...]
        for step in range(1, count):
            little_copy(step).start()
        pairs = total // 2
        ahead = 3
        stages = (finish_one, finish_two, finish_over, finish_back, finish_back_two, finish_back_one)
        for k in range(min(ahead, pairs)):
            begin_one(2 * k)
            begin_one(2 * k + 1)
        for turn in range(pairs + len(stages) - 1):
            for depth, stage in enumerate(stages):
                k = turn - depth
                if 0 <= k < pairs:
                    stage(2 * k)
                    stage(2 * k + 1)
                if depth == 0 and turn + ahead < pairs:
                    begin_one(2 * (turn + ahead))
                    begin_one(2 * (turn + ahead) + 1)
            if turn == 0:
                for step in range(1, count):
                    little_copy(step).wait()
                value = little_in[...]
                for step in range(1, count):
                    value = value + little_slots[step - 1]
                little_x[0] = value
                little_pair(0, little_x.at[0], little_x.at[1], to_x).start()
            if turn == 1:
                little_pair(0, little_x.at[0], little_x.at[1], to_x).wait()
                little_y[0] = little_x[0] + little_x[1]
                little_pair(1, little_y.at[0], little_y.at[1], to_y).start()
            if turn == 2:
                little_pair(1, little_y.at[0], little_y.at[1], to_y).wait()
                little_out[...] = little_y[0] + little_y[1]
        for b in range(total):
            stage_one(b).wait_send()
            stage_two(b).wait_send()
            for step in range(1, count):
                copy, send, take = spread(b, step)
                guarded(send, copy.wait_send)
                copy, send, take = gather(b, step)
                guarded(send, copy.wait_send)
            gather_two(b).wait_send()
            gather_one(b).wait_send()
            keep(b).wait()


def unwritten(shapes):
    return pl.pallas_call(
        lambda *refs: None,
        out_shape=[jax.ShapeDtypeStruct(shape, low) for shape in shapes],
        out_specs=[pl.BlockSpec(memory_space=pl.ANY)] * len(shapes),
    )()


def reduce_all(parts, little, ident, live):
    count = lax.axis_size(SEQ)
    tall = -(-(2 * little[0].shape[0] + len(little) - 1) // 8) * 8
    side = min(min(part.shape) for part in parts)
    across = side // 2
    blocks = []
    for k, part in enumerate(parts):
        for top in range(0, part.shape[0], side):
            for left in range(0, part.shape[1], across):
                blocks.append((k, top, left))
    total = len(blocks)
    small = side // 4
    piece = max(TAIL, small // count)
    vmem = pl.BlockSpec(memory_space=pltpu.VMEM)
    sems = pltpu.SemaphoreType.DMA
    return pl.pallas_call(
        functools.partial(reduce_kernel, count, blocks, side, across, len(parts), live),
        out_shape=[jax.ShapeDtypeStruct(part.shape, low) for part in parts]
        + [jax.ShapeDtypeStruct((tall, side), full)],
        in_specs=[pl.BlockSpec(memory_space=pl.ANY)] * len(parts) + [vmem] * len(little),
        out_specs=[pl.BlockSpec(memory_space=pl.ANY)] * len(parts) + [vmem],
        scratch_shapes=[
            pltpu.VMEM((total, side // 2, across), low),
            pltpu.VMEM((total, small, across), low),
            pltpu.VMEM((total, count - 1, piece, across), low),
            pltpu.VMEM((tall, side), full),
            pltpu.VMEM((count - 1, tall, side), full),
            pltpu.VMEM((2, tall, side), full),
            pltpu.VMEM((2, tall, side), full),
            pltpu.VMEM((total, side // 2, across), low),
            pltpu.VMEM((total, side, across), low),
            sems((2, total)),
            sems((2, total)),
            sems((2, total, count - 1)),
            sems((2, total, count - 1)),
            sems((2, total)),
            sems((2, total)),
            sems((2, count + 1)),
            sems((total,)),
            sems((total,)),
        ],
        compiler_params=pltpu.CompilerParams(
            collective_id=ident, has_side_effects=True, vmem_limit_bytes=62 << 20
        ),
    )(*parts, *little)


def layer_forward(tick, live, state_low, params, positions, count):
    qkv_w, output_w, up_w, down_w, taps, gain_one, bias_one, gain_two, bias_two = params
    rows, width = state_low.shape
    base = lax.axis_index(SEQ) * rows
    length = lax.axis_size(SEQ) * rows
    valid = jnp.arange(QMAX, dtype=jnp.int32) < count
    row_pos = base + jnp.arange(rows, dtype=jnp.int32)
    select = (positions[:, None] == row_pos[None, :]) & valid[:, None]
    select_low = select.astype(low)
    scalars = jnp.stack([base, jnp.int32(length), positions[0], count])
    pick = mm(select_low, state_low).astype(low)
    extended = gather_rows(4 * tick, live, state_low, pick)
    normed = norm_rows(extended.astype(full), gain_one, bias_one).astype(low)
    spot = base - TAIL - rows + jnp.arange(extended.shape[0], dtype=jnp.int32)
    inside = ((spot >= 0) & (spot < length)) | (jnp.arange(extended.shape[0]) >= TAIL + 3 * rows)
    qkv = jnp.where(inside[:, None], mm(normed, qkv_w), 0.0).astype(low)
    local, pooled, stats, answer, qstats = attend(4 * tick + 1, live, scalars, qkv, taps, rows)
    is_question = jnp.any(select, axis=0)
    replaced = tn(select_low, answer.astype(low))
    mixed = jnp.where(is_question[:, None], replaced, local).astype(low)
    state = state_low.astype(full)
    middle = state + mm(mixed, output_w)
    normed_two = norm_rows(middle, gain_two, bias_two).astype(low)
    hidden = mm(normed_two, up_w)
    active, slope = gelu_parts(hidden)
    result = middle + mm(active, down_w)
    tape = (state_low, select_low, scalars, normed, qkv, pooled, stats, qstats, answer, mixed,
            middle, normed_two, slope, active)
    return result.astype(low), tape


def layer_backward(tick, live, grad_low, params, tape):
    qkv_w, output_w, up_w, down_w, taps, gain_one, bias_one, gain_two, bias_two = params
    (state_low, select_low, scalars, normed, qkv, pooled, stats, qstats, answer, mixed,
     middle, normed_two, slope, active) = tape
    rows, width = state_low.shape
    grad_out = grad_low.astype(full)
    grad_active = nt(grad_low, down_w)
    grad_hidden = (grad_active * slope.astype(full)).astype(low)
    grad_normed_two = nt(grad_hidden, up_w)
    _, norm_back_two = jax.vjp(norm_rows, middle, gain_two, bias_two)
    grad_middle, g_gain_two, g_bias_two = norm_back_two(grad_normed_two)
    grad_middle = grad_middle + grad_out
    branch = grad_middle.astype(low)
    grad_mixed = nt(branch, output_w).astype(low)
    grad_part = mm(select_low, grad_mixed).astype(low)
    grads, grad_taps = attend_back(
        4 * tick + 2, live, scalars, qkv, taps, pooled, stats, qstats, answer, grad_mixed,
        grad_part, rows
    )
    grad_extended = nt(grads, qkv_w).astype(low)
    grad_normed, grad_picked = return_rows(4 * tick + 3, live, grad_extended, rows)
    grad_normed = grad_normed + tn(select_low, grad_picked.astype(low))
    _, norm_back_one = jax.vjp(norm_rows, state_low.astype(full), gain_one, bias_one)
    grad_state, g_gain_one, g_bias_one = norm_back_one(grad_normed)
    small = (grad_taps, g_gain_one, g_bias_one, g_gain_two, g_bias_two)
    big = ((normed, grads), (mixed, branch), (normed_two, grad_hidden), (active, grad_low))
    return (grad_state + grad_middle).astype(low), big, small


def to_partner(block):
    return lax.ppermute(block, SECTION, [(0, 1), (1, 0)])


def per_device(
    inputs,
    cotangent,
    question_positions,
    question_counts,
    query_weight,
    key_weight,
    value_weight,
    output_weight,
    up_weight,
    down_weight,
    key_pool,
    value_pool,
    attn_norm_gain,
    attn_norm_bias,
    ffn_norm_gain,
    ffn_norm_bias,
):
    params = (
        jnp.concatenate([query_weight[0], key_weight[0], value_weight[0]], axis=1),
        output_weight[0],
        up_weight[0],
        down_weight[0],
        jnp.concatenate([key_pool[0], value_pool[0]], axis=1),
        attn_norm_gain[0],
        attn_norm_bias[0],
        ffn_norm_gain[0],
        ffn_norm_bias[0],
    )
    section = lax.axis_index(SECTION)
    micro, rows, width = inputs.shape

    def alive(tick):
        if tick == 0:
            return 0
        return 1 if tick == micro else None

    received = jnp.zeros((rows, width), low)
    tapes = []
    made = []
    for tick in range(micro + 1):
        slot = jnp.clip(tick - section, 0, micro - 1)
        layer_in = jnp.where(section == 0, inputs[min(tick, micro - 1)], received)
        result, tape = layer_forward(
            tick, alive(tick), layer_in, params, question_positions[slot], question_counts[slot]
        )
        tapes.append(tape)
        made.append(result)
        if tick < micro:
            received = to_partner(result)
    produced = jnp.where(section == 0, jnp.stack(made[:micro]), jnp.stack(made[1:]))
    grad_in = jnp.zeros((rows, width), low)
    back = []
    bigs = []
    smalls = []
    reduced = []

    def reduce_section(which):
        ticks = range(1 - which, micro + 1 - which)

        def sums():
            parts = []
            for k in range(len(bigs[0])):
                left = jnp.concatenate([bigs[t][k][0] for t in ticks], axis=0)
                right = jnp.concatenate([bigs[t][k][1] for t in ticks], axis=0)
                parts.append(tn(left, right).astype(low))
            return parts

        def nothing():
            return list(unwritten([(a.shape[1], b.shape[1]) for a, b in bigs[micro - 1]]))

        parts = lax.cond(section == which, sums, nothing)
        little = []
        for k in range(len(smalls[0])):
            total = smalls[ticks[0]][k]
            for t in ticks[1:]:
                total = total + smalls[t][k]
            little.append(total.reshape(-1, total.shape[-1]))
        reduced.append(reduce_all(parts, little, 4 * micro + 4 + which, which))

    for tick in range(micro + 1):
        mirror = micro - tick
        grad_out = jnp.where(section == 1, cotangent[max(mirror - 1, 0)], grad_in)
        grad_state, big, small = layer_backward(
            mirror, alive(mirror), grad_out, params, tapes[mirror]
        )
        back.append(grad_state)
        bigs.append(big)
        smalls.append(small)
        if tick < micro:
            grad_in = to_partner(grad_state)
        if tick == micro - 1:
            grad_in, bigs, smalls = lax.optimization_barrier((grad_in, bigs, smalls))
            reduce_section(1)
            grad_in, reduced[0] = lax.optimization_barrier((grad_in, reduced[0]))
    back_grads = jnp.where(
        section == 0, jnp.stack(back[1:][::-1]), jnp.stack(back[:micro][::-1])
    )
    reduce_section(0)
    taps = key_pool.shape[1]

    def finished(parts):
        *sums, little = [part.astype(full) for part in parts]
        return (
            sums[0][:, :width],
            sums[0][:, width : 2 * width],
            sums[0][:, 2 * width :],
            sums[1],
            sums[2],
            sums[3],
            little[:taps],
            little[taps : 2 * taps],
        ) + tuple(little[2 * taps + k] for k in range(4))

    outs = lax.cond(
        section == 0,
        lambda early, late: finished(late),
        lambda early, late: finished(early),
        *reduced,
    )
    return (produced[None], back_grads[None]) + tuple(out[None] for out in outs)


def solution(mesh):
    rows = P(DP, SEQ, None)
    matrix = P(SECTION, None, None)
    vector = P(SECTION, None)
    result = P(SECTION, DP, SEQ, None)
    return jax.shard_map(
        per_device,
        mesh=mesh,
        in_specs=(rows, rows, P(DP, None), P(DP)) + (matrix,) * 8 + (vector,) * 4,
        out_specs=(result, result) + (matrix,) * 8 + (vector,) * 4,
        check_vma=False,
    )
```
